32 devices in a mesh: gz: 4 (over x, core), gy: 8 (over z, y).
Axes of the slice: x: 2, y: 2, z: 4, core: 2. Of those that a mesh axis runs over, the one named last changes fastest.
Arguments:
- zone_ids: int32 [32, 256, 512], P('gz', 'gy'), may hold values from 0 to 7
- fixed_cells: int32 [32, 256, 512], P('gz', 'gy'), may hold values 0 or 1
- pressure_old: float32 [32, 256, 512], P('gz', 'gy'), may hold values from -6 to 6
- pressure_iter: float32 [32, 256, 512], P('gz', 'gy'), may hold values from -6 to 6
- strain_change: float32 [32, 256, 512], P('gz', 'gy'), may hold values from -3 to 3
- source: float32 [32, 256, 512], P('gz', 'gy'), may hold values from -40 to 40
- zone_perm: float32 [8], replicated, may hold values from 0.2 to 5
- zone_storage: float32 [8], replicated, may hold values from 0.1 to 1
- zone_biot: float32 [8], replicated, may hold values from 0.5 to 1
- zone_bulk: float32 [8], replicated, may hold values from 0.5 to 2
Outputs:
- pressure: float32 [32, 256, 512], P('gz', 'gy')
- strain_next: float32 [32, 256, 512], P('gz', 'gy')
- outer_norms: float32 [2], replicated
The draws below stay inside these ranges and needn't reach their ends.
All inputs are finite; a program needn't handle non-finite values. No bound on the sum of `fixed_cells` on one device may be relied on, other than what follows from the above.
Results may differ from the reference program's by a relative error of at most 0.00016.
Values sent between devices are 32-bit elements; how exact they have to be, the bound alone decides.
No kernel may reach another device: no remote copies, remote signals or barrier semaphores. Data moves between devices by JAX's collectives and lax.ppermute only.
A program may use at most 64 MiB of HBM per device.

```python
import math
import jax
import jax.numpy as jnp

NX = 512
ITERS = 3
ZONES = 8
NZ = 32
NY = 256
CELLS = 4194304


def draw_source(key, part):
    rough_key = jax.random.fold_in(jax.random.fold_in(key, 17), 0)
    z_position = (jnp.arange(NZ, dtype=jnp.float32) / max(NZ - 1, 1))[:, None, None]
    y_position = (jnp.arange(NY, dtype=jnp.float32) / max(NY - 1, 1))[None, :, None]
    ramp_scale = 1.0 + z_position + y_position
    rough_part = jax.random.truncated_normal(rough_key, -4.0, 4.0, (NZ, NY, NX), jnp.float32)
    return rough_part * ramp_scale


def touch_ends(entries, stream_key, low, largest):
    place = [jax.random.randint(jax.random.fold_in(stream_key, axis), (), 0, length) for axis, length in enumerate(entries.shape)]
    main_axis = entries.shape.index(max(entries.shape))
    beside = place[:main_axis] + [(place[main_axis] + 1) % entries.shape[main_axis]] + place[main_axis + 1:]
    return entries.at[tuple(place)].set(low).at[tuple(beside)].set(largest)


def block_levels(key, extent, cuts, least, largest):
    loudness, own = 1.0, jax.random.fold_in(key, 6)
    for position, parts in cuts:
        steps = jnp.exp(jax.random.uniform(jax.random.fold_in(own, position), (parts,), jnp.float32, least / len(cuts), largest / len(cuts)))
        loudness = loudness * jnp.repeat(steps, extent[position] // parts).reshape([-1 if axis == position else 1 for axis in range(len(extent))])
    return loudness


def normal_values(key, dims, deviation, bound, shards=(), kind=jnp.bfloat16):
    entries = jax.random.normal(key, dims, jnp.float32) * deviation
    if len(shards) > 0:
        entries = block_levels(key, dims, shards, -0.22, 0.18) * entries
    return jnp.clip(entries, min=-bound, max=bound).astype(kind)


def setup_inputs(seed: int = 0) -> dict:
    key_of = jax.random.split(jax.random.key(seed), 11)
    return {
        "zone_ids": touch_ends(jax.random.randint(key_of[0], (NZ, NY, NX), 0, ZONES), jax.random.fold_in(key_of[0], 1), 0, ZONES - 1).astype(jnp.int32),
        "fixed_cells": touch_ends((jax.random.randint(key_of[1], (NZ, NY, NX), 0, 16) < 1).astype(jnp.int32), jax.random.fold_in(key_of[1], 1), 0, 1),
        "pressure_old": normal_values(key_of[2], (NZ, NY, NX), 1.0, 6.0, ((0, 4), (1, 8)), jnp.float32),
        "pressure_iter": normal_values(key_of[3], (NZ, NY, NX), 1.0, 6.0, ((0, 4), (1, 8)), jnp.float32),
        "strain_change": normal_values(key_of[4], (NZ, NY, NX), 0.5, 3.0, ((0, 4), (1, 8)), jnp.float32),
        "source": draw_source(jax.random.fold_in(key_of[10], 71), 0),
        "zone_perm": jnp.clip(jnp.exp(jax.random.uniform(key_of[6], (ZONES,), jnp.float32, math.log(0.2), math.log(5.0))), 0.2, 5.0),
        "zone_storage": jnp.clip(jnp.exp(jax.random.uniform(key_of[7], (ZONES,), jnp.float32, math.log(0.1), math.log(1.0))), 0.1, 1.0),
        "zone_biot": jnp.clip(jax.random.uniform(key_of[8], (ZONES,), jnp.float32, 0.5, 1.0), 0.5, 1.0),
        "zone_bulk": jnp.clip(jnp.exp(jax.random.uniform(key_of[9], (ZONES,), jnp.float32, math.log(0.5), math.log(2.0))), 0.5, 2.0),
    }


def lookup(zone_ids, zone_table):
    result = jnp.zeros(zone_ids.shape, jnp.float32)
    for zone_index in range(zone_table.shape[0]):
        result = jnp.where(zone_ids == zone_index, zone_table[zone_index], result)
    return result

def harmonic(lower_side, upper_side):
    return 2.0 * lower_side * upper_side / (lower_side + upper_side)

def neighbour_views(padded):
    return (padded[:-2, 1:-1, 1:-1], padded[2:, 1:-1, 1:-1], padded[1:-1, :-2, 1:-1], padded[1:-1, 2:, 1:-1], padded[1:-1, 1:-1, :-2], padded[1:-1, 1:-1, 2:])

def reference(zone_ids, fixed_cells, pressure_old, pressure_iter, strain_change, source, zone_perm, zone_storage, zone_biot, zone_bulk):
    storage = lookup(zone_ids, zone_storage)
    biot_coeff = lookup(zone_ids, zone_biot)
    bulk_modulus = lookup(zone_ids, zone_bulk)
    permeability = lookup(zone_ids, zone_perm)
    coupling = biot_coeff * biot_coeff / bulk_modulus
    face_terms = tuple((harmonic(permeability, view) for view in neighbour_views(jnp.pad(permeability, 1))))
    diagonal = storage + coupling
    for face in face_terms:
        diagonal = diagonal + face
    free_cells = 1.0 - fixed_cells.astype(jnp.float32)

    def operator(values):
        views = neighbour_views(jnp.pad(values, 1))
        neighbours = face_terms[0] * views[0]
        for number in range(1, 6):
            neighbours = neighbours + face_terms[number] * views[number]
        return diagonal * values - neighbours
    right_side = storage * pressure_old + coupling * pressure_iter - biot_coeff * strain_change + source
    pressure = pressure_iter
    residual = free_cells * (right_side - operator(pressure_iter))
    precond = residual / diagonal
    direction = precond
    inner_now = jnp.sum(residual * precond)
    for step_index in range(ITERS):
        applied = free_cells * operator(direction)
        step_size = inner_now / jnp.sum(direction * applied)
        pressure = pressure + step_size * direction
        residual = residual - step_size * applied
        if step_index + 1 < ITERS:
            precond = residual / diagonal
            inner_next = jnp.sum(residual * precond)
            direction = precond + inner_next / inner_now * direction
            inner_now = inner_next
    change = biot_coeff / bulk_modulus * (pressure - pressure_iter)
    strain_next = strain_change + change
    closing = free_cells * (right_side - operator(pressure))
    outer_norms = jnp.sqrt(jnp.stack([jnp.sum(closing * closing), jnp.sum(change * change)]) / CELLS)
    return (pressure, strain_next, outer_norms)
```

```python
import functools

import jax
import jax.numpy as jnp
from jax import lax
from jax.experimental import pallas as pl
from jax.experimental.pallas import tpu as pltpu
from jax.sharding import PartitionSpec as P

F32 = jnp.float32
ROWS = 8
LANES = 128
VMEM = pl.BlockSpec(memory_space=pltpu.VMEM)
SMEM = pl.BlockSpec(memory_space=pltpu.SMEM)

MOMENTS = (("q", 0, "u", 0), ("q", 0, "u", 1), ("q", 1, "u", 1), ("q", 1, "u", 2), ("q", 2, "u", 2), ("q", 2, "u", 3))
CLOSING = tuple(("u", i, "u", j) for i in range(4) for j in range(i, 4))
CHANGE = tuple(("y", i, "y", j) for i in range(3) for j in range(i, 3))
SUMS = MOMENTS + CLOSING + CHANGE
EARLY = tuple(s for s in SUMS if max(s[1], s[3]) <= 1)
MIDDLE = tuple(s for s in SUMS if max(s[1], s[3]) == 2)
LATE = tuple(s for s in SUMS if max(s[1], s[3]) == 3)


def table_row(table_ref):
    lane = lax.broadcasted_iota(jnp.int32, (ROWS, LANES), 1)
    row = jnp.zeros((ROWS, LANES), F32)
    for zone in range(table_ref.shape[0]):
        row = jnp.where(lane == zone, table_ref[zone], row)
    return row


def look_up(row, zones):
    parts = [
        jnp.take_along_axis(row, zones[:, at : at + LANES], axis=1, mode="promise_in_bounds")
        for at in range(0, zones.shape[1], LANES)
    ]
    return jnp.concatenate(parts, axis=1)


def harmonic(lower_side, upper_side):
    return 2.0 * lower_side * upper_side / (lower_side + upper_side)


def row_shifts(tiles, before, after):
    sub = lax.broadcasted_iota(jnp.int32, tiles[0].shape, 0)
    down = [pltpu.roll(tile, 1, 0) for tile in tiles]
    up = [pltpu.roll(tile, ROWS - 1, 0) for tile in tiles]
    lower, upper = [], []
    for at in range(len(tiles)):
        lower.append(jnp.where(sub == 0, down[at - 1] if at else before, down[at]))
        upper.append(jnp.where(sub == ROWS - 1, up[at + 1] if at + 1 < len(tiles) else after, up[at]))
    return lower, upper


def lane_shifts(tile):
    width = tile.shape[1]
    return pltpu.roll(tile, 1, 1), pltpu.roll(tile, width - 1, 1)


def pack_kernel(zone_ref, pressure_ref, perm_table, z_low, z_high, y_low, y_high):
    planes, rows, _ = zone_ref.shape
    perm_row = table_row(perm_table)
    for plane, out in ((0, z_low), (planes - 1, z_high)):
        for at in range(0, rows, ROWS):
            part = pl.ds(at, ROWS)
            out[0, part] = look_up(perm_row, zone_ref[plane, part])
        out[1] = pressure_ref[plane]
    for row, out in ((0, y_low), (rows - 1, y_high)):
        for plane in range(planes):
            out[1, pl.ds(plane, 1)] = pressure_ref[plane, pl.ds(row, 1)]
        zones = jnp.concatenate([zone_ref[plane, pl.ds(row, 1)] for plane in range(planes)], axis=0)
        out[0] = look_up(perm_row, zones)


def write_faces(values, z, at, planes, rows, z_low, z_high, y_low, y_high):
    if at == 0:
        y_low[pl.ds(z, 1)] = values[:1]
    if at == rows - ROWS:
        y_high[pl.ds(z, 1)] = values[ROWS - 1 :]


def setup_kernel(
    zone_ref, fixed_ref, old_ref, pressure_ref, strain_ref, source_ref,
    perm_table, storage_table, biot_table, bulk_table,
    below_z, above_z, below_y, above_y,
    faces, inverse, ratio, q_out, u_out, z_low, z_high, y_low, y_high,
    perm,
):
    planes, rows, width = zone_ref.shape
    gz, gy = lax.axis_index("gz"), lax.axis_index("gy")
    inside = [
        jnp.where(test, 1.0, 0.0).astype(F32)
        for test in (gz > 0, gz < lax.axis_size("gz") - 1, gy > 0, gy < lax.axis_size("gy") - 1)
    ]
    perm_row = table_row(perm_table)
    storage_row = table_row(storage_table)
    biot_row = table_row(biot_table)
    bulk_row = jnp.where(lax.broadcasted_iota(jnp.int32, (ROWS, LANES), 1) < bulk_table.shape[0], table_row(bulk_table), 1.0)
    ratio_row = biot_row / bulk_row
    coupling_row = biot_row * biot_row / bulk_row
    lane = lax.broadcasted_iota(jnp.int32, (ROWS, width), 1)
    perm[0] = below_z[0] * inside[0]
    perm[planes + 1] = above_z[0] * inside[1]

    def fill(z, carry):
        for at in range(0, rows, ROWS):
            part = pl.ds(at, ROWS)
            perm[z + 1, part] = look_up(perm_row, zone_ref[z, part])
        return carry

    lax.fori_loop(0, planes, fill, 0)

    def plane(z, low_pressure, high_pressure):
        parts = [pl.ds(at, ROWS) for at in range(0, rows, ROWS)]
        perms = [perm[z + 1, part] for part in parts]
        values = [pressure_ref[z, part] for part in parts]
        one = pl.ds(z, 1)
        full = (ROWS, width)
        perm_lower, perm_upper = row_shifts(
            perms,
            jnp.broadcast_to(below_y[0, one] * inside[2], full),
            jnp.broadcast_to(above_y[0, one] * inside[3], full),
        )
        value_lower, value_upper = row_shifts(
            values, jnp.broadcast_to(below_y[1, one], full), jnp.broadcast_to(above_y[1, one], full)
        )
        for at, part in enumerate(parts):
            zones = zone_ref[z, part]
            storage = look_up(storage_row, zones)
            coupling = look_up(coupling_row, zones)
            biot = look_up(biot_row, zones)
            ratio[z, part] = look_up(ratio_row, zones)
            here, value = perms[at], values[at]
            x_lower, x_upper = lane_shifts(here)
            x_lower = jnp.where(lane == 0, 0.0, x_lower)
            x_upper = jnp.where(lane == width - 1, 0.0, x_upper)
            value_left, value_right = lane_shifts(value)
            beside = (perm[z, part], perm[z + 2, part], perm_lower[at], perm_upper[at], x_lower, x_upper)
            terms = [harmonic(here, other) for other in beside]
            free = 1.0 - fixed_ref[z, part].astype(F32)
            diagonal = storage + coupling
            for term in terms:
                diagonal = diagonal + term
            views = (low_pressure[part], high_pressure[part], value_lower[at], value_upper[at], value_left, value_right)
            neighbours = terms[0] * views[0]
            for number in range(1, 6):
                neighbours = neighbours + terms[number] * views[number]
            right_side = (
                storage * old_ref[z, part] + coupling * value - biot * strain_ref[z, part] + source_ref[z, part]
            )
            residual = free * (right_side - (diagonal * value - neighbours))
            reciprocal = 1.0 / diagonal
            precond = residual * reciprocal
            for number in range(6):
                faces[number, z, part] = free * terms[number]
            inverse[z, part] = reciprocal
            u_out[z, part] = residual
            q_out[z, part] = precond
            write_faces(precond, z, part.start, planes, rows, z_low, z_high, y_low, y_high)

    plane(0, below_z.at[1], pressure_ref.at[1])
    lax.fori_loop(1, planes - 1, lambda z, c: (plane(z, pressure_ref.at[z - 1], pressure_ref.at[z + 1]), c)[1], 0)
    plane(planes - 1, pressure_ref.at[planes - 2], above_z.at[1])
    z_low[...] = q_out[0]
    z_high[...] = q_out[planes - 1]


def apply_plane(z, low, high, q_ref, faces, inverse, below_y, above_y, emit):
    rows, width = q_ref.shape[1:]
    parts = [pl.ds(at, ROWS) for at in range(0, rows, ROWS)]
    values = [q_ref[z, part] for part in parts]
    one, full = pl.ds(z, 1), (ROWS, width)
    lower, upper = row_shifts(
        values, jnp.broadcast_to(below_y[one], full), jnp.broadcast_to(above_y[one], full)
    )
    for at, part in enumerate(parts):
        left, right = lane_shifts(values[at])
        u = faces[0, z, part] * low[part] + faces[1, z, part] * high[part]
        u = u + faces[2, z, part] * lower[at] + faces[3, z, part] * upper[at]
        u = u + faces[4, z, part] * left + faces[5, z, part] * right
        emit(part, u, u * inverse[z, part])


def over_planes(planes, q_ref, below_z, above_z, body, carry):
    carry = body(0, below_z, q_ref.at[1], carry)
    carry = lax.fori_loop(1, planes - 1, lambda z, c: body(z, q_ref.at[z - 1], q_ref.at[z + 1], c), carry)
    return body(planes - 1, q_ref.at[planes - 2], above_z, carry)


def stage_kernel(
    q_ref, faces, inverse, below_z, above_z, below_y, above_y,
    q_out, u_out, z_low, z_high, y_low, y_high,
):
    planes, rows, _ = q_ref.shape

    def body(z, low, high, carry):
        def emit(part, u, q):
            u_out[z, part] = u
            q_out[z, part] = q
            write_faces(q, z, part.start, planes, rows, z_low, z_high, y_low, y_high)

        apply_plane(z, low, high, q_ref, faces, inverse, below_y, above_y, emit)
        return carry

    over_planes(planes, q_ref, below_z, above_z, body, 0)
    z_low[...] = q_out[0]
    z_high[...] = q_out[planes - 1]


def fold(product):
    total = product[:, :LANES]
    for at in range(LANES, product.shape[1], LANES):
        total = total + product[:, at : at + LANES]
    return total


def gram_kernel(sums, count, *refs):
    us, qs = refs[: count], refs[count : 2 * count]
    ratio, out = refs[2 * count :]
    planes, rows, _ = ratio.shape

    def body(z, totals):
        totals = list(totals)
        for at in range(0, rows, ROWS):
            part = pl.ds(at, ROWS)
            fields = {("u", i): us[i][z, part] for i in range(count)}
            fields |= {("q", i): qs[i][z, part] for i in range(count)}
            weight = ratio[z, part]
            fields |= {("y", i): weight * fields["q", i] for i in range(count)}
            for number, (a, i, b, j) in enumerate(sums):
                totals[number] = totals[number] + fold(fields[a, i] * fields[b, j])
        return tuple(totals)

    zero = jnp.zeros((ROWS, LANES), F32)
    for number, total in enumerate(lax.fori_loop(0, planes, body, (zero,) * len(sums))):
        out[number] = total


def last_kernel(
    q2_ref, faces, inverse, u0_ref, u1_ref, u2_ref, below_z, above_z, below_y, above_y, early, middle, out
):
    planes = q2_ref.shape[0]
    us = (u0_ref, u1_ref, u2_ref)

    def body(z, low, high, totals):
        totals = list(totals)

        def emit(part, u3, _):
            fields = {("u", i): us[i][z, part] for i in range(3)}
            fields |= {("u", 3): u3, ("q", 2): q2_ref[z, part]}
            for number, (a, i, b, j) in enumerate(LATE):
                totals[number] = totals[number] + fold(fields[a, i] * fields[b, j])

        apply_plane(z, low, high, q2_ref, faces, inverse, below_y, above_y, emit)
        return tuple(totals)

    zero = jnp.zeros((ROWS, LANES), F32)
    late = over_planes(planes, q2_ref, below_z, above_z, body, (zero,) * len(LATE))
    lane = lax.broadcasted_iota(jnp.int32, (1, LANES), 1)
    row = jnp.zeros((1, LANES), F32)
    for names, totals in ((EARLY, early), (MIDDLE, middle), (LATE, late)):
        for number, name in enumerate(names):
            row = jnp.where(lane == SUMS.index(name), jnp.sum(totals[number], keepdims=True), row)
    out[...] = jnp.broadcast_to(row, out.shape)


def quadratic(left, table, right):
    total = None
    for i, a in enumerate(left):
        for j, b in enumerate(right):
            if a is None or b is None:
                continue
            term = a * b * table(i, j)
            total = term if total is None else total + term
    return total


def combine(totals, cell_count, iterations=3):
    moment = lambda i, j: totals[i + j]
    drop = lambda i, j: totals[i + j] - totals[i + j + 1]
    zero = jnp.zeros_like(totals[0])
    one = zero + 1.0
    residual, direction, change = [one], [one], []
    inner = moment(0, 0)
    for step in range(iterations):
        curvature = quadratic(direction, drop, direction)
        alive = (inner > 0.0) & (curvature > 0.0)
        size = jnp.where(alive, inner / jnp.where(alive, curvature, 1.0), 0.0)
        change = [c + size * d for c, d in zip(change + [zero], direction)]
        image = [a - b for a, b in zip(direction + [zero], [zero] + direction)]
        residual = [r - size * a for r, a in zip(residual + [zero], image)]
        if step + 1 < iterations:
            following = quadratic(residual, moment, residual)
            noise = quadratic([abs(r) for r in residual], lambda i, j: abs(moment(i, j)), [abs(r) for r in residual])
            following = jnp.where(following > 1e-7 * noise, following, 0.0)
            growth = jnp.where(inner > 0.0, following / jnp.where(inner > 0.0, inner, 1.0), 0.0)
            direction = [z + growth * d for z, d in zip(residual, direction + [zero])]
            inner = following
    at = {name: total for name, total in zip(SUMS, totals)}
    closing = quadratic(residual, lambda i, j: at["u", min(i, j), "u", max(i, j)], residual)
    changed = quadratic(change, lambda i, j: at["y", min(i, j), "y", max(i, j)], change)
    scale = 1.0 / cell_count
    return change, jnp.sqrt(jnp.maximum(closing, 0.0) * scale), jnp.sqrt(jnp.maximum(changed, 0.0) * scale)


def final_kernel(cell_count, rows_ref, q0, q1, q2, pressure_ref, strain_ref, ratio, pressure_out, strain_out, norms):
    planes, rows, width = pressure_ref.shape
    lane = lax.broadcasted_iota(jnp.int32, (1, LANES), 1)
    row = jnp.sum(rows_ref[...], axis=0, keepdims=True)
    totals = [jnp.sum(jnp.where(lane == at, row, 0.0), axis=1, keepdims=True) for at in range(len(SUMS))]
    change, closing, changed = combine(totals, cell_count)
    norms[...] = jnp.where(lane == 0, closing, changed)[:, :2]
    weights = [jnp.broadcast_to(c, (ROWS, width)) for c in change]

    def body(z, carry):
        for at in range(0, rows, ROWS):
            part = pl.ds(at, ROWS)
            delta = weights[0] * q0[z, part] + weights[1] * q1[z, part] + weights[2] * q2[z, part]
            pressure_out[z, part] = pressure_ref[z, part] + delta
            strain_out[z, part] = strain_ref[z, part] + ratio[z, part] * delta
        return carry

    lax.fori_loop(0, planes, body, 0)


def ring(axis, step):
    count = lax.axis_size(axis)
    return [(i, (i + step) % count) for i in range(count)]


def exchange(z_low, z_high, y_low, y_high):
    return (
        lax.ppermute(z_high, "gz", ring("gz", 1)),
        lax.ppermute(z_low, "gz", ring("gz", -1)),
        lax.ppermute(y_high, "gy", ring("gy", 1)),
        lax.ppermute(y_low, "gy", ring("gy", -1)),
    )


def call(kernel, name, outs, specs, *operands, scratch=()):
    shapes = [jax.ShapeDtypeStruct(shape, F32) for shape in outs]
    single = len(shapes) == 1
    return pl.pallas_call(
        kernel,
        name=name,
        out_shape=shapes[0] if single else shapes,
        in_specs=specs,
        out_specs=VMEM if single else [VMEM] * len(shapes),
        scratch_shapes=list(scratch),
    )(*operands)


def per_device(
    zone_ids, fixed_cells, pressure_old, pressure_iter, strain_change, source,
    zone_perm, zone_storage, zone_biot, zone_bulk,
):
    planes, rows, width = zone_ids.shape
    field = (planes, rows, width)
    sides = ((rows, width), (rows, width), (planes, width), (planes, width))
    devices = lax.axis_size("gz") * lax.axis_size("gy")
    cell_count = zone_ids.size * devices

    packed = call(
        pack_kernel, "pack", [(2, *side) for side in sides], [VMEM, VMEM, SMEM], zone_ids, pressure_iter, zone_perm
    )
    halo = exchange(*packed)
    faces, inverse, ratio, q0, u0, *edges = call(
        setup_kernel, "setup", [(6, *field), field, field, field, field, *sides],
        [VMEM] * 6 + [SMEM] * 4 + [VMEM] * 4,
        zone_ids, fixed_cells, pressure_old, pressure_iter, strain_change, source,
        zone_perm, zone_storage, zone_biot, zone_bulk, *halo,
        scratch=[pltpu.VMEM((planes + 2, rows, width), F32)],
    )
    halo = exchange(*edges)
    q1, u1, *edges = call(stage_kernel, "stage", [field, field, *sides], [VMEM] * 7, q0, faces, inverse, *halo)
    halo = exchange(*edges)
    early = call(
        functools.partial(gram_kernel, EARLY, 2), "gram_early", [(len(EARLY), ROWS, LANES)], [VMEM] * 5,
        u0, u1, q0, q1, ratio,
    )
    q2, u2, *edges = call(stage_kernel, "stage", [field, field, *sides], [VMEM] * 7, q1, faces, inverse, *halo)
    halo = exchange(*edges)
    middle = call(
        functools.partial(gram_kernel, MIDDLE, 3), "gram_middle", [(len(MIDDLE), ROWS, LANES)], [VMEM] * 7,
        u0, u1, u2, q0, q1, q2, ratio,
    )
    sums = call(
        last_kernel, "last", [(devices, LANES)], [VMEM] * 12,
        q2, faces, inverse, u0, u1, u2, *halo, early, middle,
    )
    gathered = lax.all_to_all(sums, ("gz", "gy"), 0, 0, tiled=True)
    pressure, strain_next, norms = call(
        functools.partial(final_kernel, cell_count), "final", [field, field, (1, 2)], [VMEM] * 7,
        gathered, q0, q1, q2, pressure_iter, strain_change, ratio,
    )
    return pressure, strain_next, norms.reshape(2)


def solution(mesh):
    split = P("gz", "gy", None)
    return jax.shard_map(
        per_device,
        mesh=mesh,
        in_specs=(split,) * 6 + (P(),) * 4,
        out_specs=(split, split, P()),
        check_vma=False,
    )
```

```python
import functools

import jax
import jax.numpy as jnp
from jax import lax
from jax.experimental import pallas as pl
from jax.experimental.pallas import tpu as pltpu
from jax.sharding import PartitionSpec as P

F32 = jnp.float32
ROWS = 8
LANES = 128
VMEM = pl.BlockSpec(memory_space=pltpu.VMEM)
HBM = pl.BlockSpec(memory_space=pltpu.HBM)

MOMENTS = (("q", 0, "u", 0), ("q", 0, "u", 1), ("q", 1, "u", 1), ("q", 1, "u", 2), ("q", 2, "u", 2), ("q", 2, "u", 3))
CLOSING = tuple(("u", i, "u", j) for i in range(4) for j in range(i, 4))
CHANGE = tuple(("y", i, "y", j) for i in range(3) for j in range(i, 3))
SUMS = MOMENTS + CLOSING + CHANGE
EARLY = tuple(s for s in SUMS if max(s[1], s[3]) <= 1)
MIDDLE = tuple(s for s in SUMS if max(s[1], s[3]) == 2)
LATE = tuple(s for s in SUMS if max(s[1], s[3]) == 3)


def table_row(table_ref):
    lane = lax.broadcasted_iota(jnp.int32, (ROWS, LANES), 1)
    row = jnp.zeros((ROWS, LANES), F32)
    for zone in range(table_ref.shape[0]):
        row = jnp.where(lane == zone, table_ref[zone], row)
    return row


def look_up(row, zones):
    parts = [
        jnp.take_along_axis(row, zones[:, at : at + LANES], axis=1, mode="promise_in_bounds")
        for at in range(0, zones.shape[1], LANES)
    ]
    return jnp.concatenate(parts, axis=1)


def harmonic(lower_side, upper_side):
    return 2.0 * lower_side * upper_side / (lower_side + upper_side)


def row_shifts(tiles, before, after):
    sub = lax.broadcasted_iota(jnp.int32, tiles[0].shape, 0)
    down = [pltpu.roll(tile, 1, 0) for tile in tiles]
    up = [pltpu.roll(tile, ROWS - 1, 0) for tile in tiles]
    lower, upper = [], []
    for at in range(len(tiles)):
        lower.append(jnp.where(sub == 0, down[at - 1] if at else before, down[at]))
        upper.append(jnp.where(sub == ROWS - 1, up[at + 1] if at + 1 < len(tiles) else after, up[at]))
    return lower, upper


def lane_shifts(tile):
    width = tile.shape[1]
    return pltpu.roll(tile, 1, 1), pltpu.roll(tile, width - 1, 1)


def paired(count_z, count_y):
    return count_z % 2 == 0 and count_y % 2 == 0


def to_send(low, high):
    if not paired(lax.axis_size("gz"), lax.axis_size("gy")):
        return high, low
    odd = lax.rem(lax.axis_index("gy"), 2) == 1
    return jnp.where(odd, low, high), jnp.where(odd, high, low)


def as_sides(first, second):
    if not paired(lax.axis_size("gz"), lax.axis_size("gy")):
        return first, second
    odd = lax.rem(lax.axis_index("gy"), 2) == 1
    return jnp.where(odd, first, second), jnp.where(odd, second, first)


def inside_flags():
    flags = []
    for axis in ("gz", "gy"):
        place = lax.axis_index(axis)
        flags += [place > 0, place < lax.axis_size(axis) - 1]
    return [jnp.where(flag, 1.0, 0.0).astype(F32) for flag in flags]


def row_parts(rows):
    return [pl.ds(at, ROWS) for at in range(0, rows, ROWS)]


def pack_kernel(
    zone_hbm, pressure_hbm, perm_hbm, z_low, z_high, y_first, y_second, zone_z, zone_y, pressure_y, perm_table, sems
):
    planes, rows, _ = zone_hbm.shape
    ends = ((0, pl.ds(0, ROWS)), (planes - 1, pl.ds(rows - ROWS, ROWS)))
    copies = [pltpu.make_async_copy(perm_hbm, perm_table, sems.at[8])]
    for side, (plane, part) in enumerate(ends):
        out = (z_low, z_high)[side]
        for source, target in (
            (zone_hbm.at[plane], zone_z.at[side]),
            (pressure_hbm.at[plane], out.at[1]),
            (zone_hbm.at[:, part], zone_y.at[side]),
            (pressure_hbm.at[:, part], pressure_y.at[side]),
        ):
            copies.append(pltpu.make_async_copy(source, target, sems.at[len(copies) - 1]))
    for copy in copies:
        copy.start()
    copies[0].wait()
    perm_row = table_row(perm_table)
    for copy in copies[1:]:
        copy.wait()
    faces_y = []
    for side, out in enumerate((z_low, z_high)):
        for part in row_parts(rows):
            out[0, part] = look_up(perm_row, zone_z[side, part])
        row = pl.ds((0, ROWS - 1)[side], 1)
        zones = jnp.concatenate([zone_y[side, plane, row] for plane in range(planes)], axis=0)
        values = jnp.concatenate([pressure_y[side, plane, row] for plane in range(planes)], axis=0)
        faces_y.append((look_up(perm_row, zones), values))
    for number in range(2):
        y_first[number], y_second[number] = to_send(faces_y[0][number], faces_y[1][number])


def prepare_kernel(
    zone_hbm, fixed_hbm, old_hbm, pressure_hbm, strain_hbm, source_hbm,
    perm_hbm, storage_hbm, biot_hbm, bulk_hbm,
    faces, perm, diagonal_out, residual_out, free_out, ratio, pressure, strain,
    zone, fixed, old, source, perm_table, storage_table, biot_table, bulk_table, sems,
):
    planes, rows, width = zone_hbm.shape
    pairs = (
        (perm_hbm, perm_table), (storage_hbm, storage_table), (biot_hbm, biot_table), (bulk_hbm, bulk_table),
        (zone_hbm, zone), (pressure_hbm, pressure), (old_hbm, old), (strain_hbm, strain), (source_hbm, source),
        (fixed_hbm, fixed),
    )
    copies = [pltpu.make_async_copy(*pair, sems.at[number]) for number, pair in enumerate(pairs)]
    for copy in copies:
        copy.start()
    for copy in copies[:4]:
        copy.wait()
    perm_row = table_row(perm_table)
    storage_row = table_row(storage_table)
    biot_row = table_row(biot_table)
    known = lax.broadcasted_iota(jnp.int32, (ROWS, LANES), 1) < bulk_table.shape[0]
    bulk_row = jnp.where(known, table_row(bulk_table), 1.0)
    ratio_row = biot_row / bulk_row
    coupling_row = biot_row * biot_row / bulk_row
    lane = lax.broadcasted_iota(jnp.int32, (ROWS, width), 1)
    copies[4].wait()

    def fill(z, carry):
        for part in row_parts(rows):
            perm[z, part] = look_up(perm_row, zone[z, part])
        return carry

    lax.fori_loop(0, planes, fill, 0)
    for copy in copies[5:]:
        copy.wait()
    closed = jnp.zeros((ROWS, width), F32)

    def plane(z, low, high):
        parts = row_parts(rows)
        perms = [perm[z, part] for part in parts]
        values = [pressure[z, part] for part in parts]
        perm_lower, perm_upper = row_shifts(perms, closed, closed)
        value_lower, value_upper = row_shifts(values, closed, closed)
        for at, part in enumerate(parts):
            zones = zone[z, part]
            storage = look_up(storage_row, zones)
            coupling = look_up(coupling_row, zones)
            biot = look_up(biot_row, zones)
            ratio[z, part] = look_up(ratio_row, zones)
            here, value = perms[at], values[at]
            x_lower, x_upper = lane_shifts(here)
            x_lower = jnp.where(lane == 0, 0.0, x_lower)
            x_upper = jnp.where(lane == width - 1, 0.0, x_upper)
            value_left, value_right = lane_shifts(value)
            beside = (
                closed if low is None else perm[low, part], closed if high is None else perm[high, part],
                perm_lower[at], perm_upper[at], x_lower, x_upper,
            )
            views = (
                closed if low is None else pressure[low, part], closed if high is None else pressure[high, part],
                value_lower[at], value_upper[at], value_left, value_right,
            )
            terms = [harmonic(here, other) for other in beside]
            free = 1.0 - fixed[z, part].astype(F32)
            diagonal = storage + coupling
            for term in terms:
                diagonal = diagonal + term
            neighbours = terms[0] * views[0]
            for number in range(1, 6):
                neighbours = neighbours + terms[number] * views[number]
            right_side = storage * old[z, part] + coupling * value - biot * strain[z, part] + source[z, part]
            for number in range(6):
                faces[number, z, part] = free * terms[number]
            diagonal_out[z, part] = diagonal
            residual_out[z, part] = right_side - (diagonal * value - neighbours)
            free_out[z, part] = free

    plane(0, None, 1)
    lax.fori_loop(1, planes - 1, lambda z, c: (plane(z, z - 1, z + 1), c)[1], 0)
    plane(planes - 1, planes - 2, None)


def begin_kernel(
    perm, diagonal_ref, residual_ref, free_ref, pressure, below_z, above_z, y_got, y_got_too,
    inverse, q_out, u_out, face_z, face_y, z_low, z_high, y_first, y_second,
    y_low, y_high,
):
    planes, rows, width = pressure.shape
    inside = inside_flags()
    below_perm, above_perm = as_sides(y_got[0], y_got_too[0])
    below_value, above_value = as_sides(y_got[1], y_got_too[1])
    below_perm, above_perm = below_perm * inside[2], above_perm * inside[3]
    sub = lax.broadcasted_iota(jnp.int32, (ROWS, width), 0)
    ends = (
        (pl.ds(0, 1), below_perm, below_value),
        (pl.ds(rows - 1, 1), above_perm, above_value),
    )
    gain_y = []
    for side, (row, other, value) in enumerate(ends):
        here = jnp.concatenate([perm[z, row] for z in range(planes)], axis=0)
        own = jnp.concatenate([pressure[z, row] for z in range(planes)], axis=0)
        free = jnp.concatenate([free_ref[z, row] for z in range(planes)], axis=0)
        term = harmonic(here, other)
        face_y[side] = free * term
        gain_y.append((term, term * (value - own)))

    def plane(z, outer):
        for part in row_parts(rows):
            diagonal, residual, free = diagonal_ref[z, part], residual_ref[z, part], free_ref[z, part]
            if outer is not None:
                side, halo = outer
                term = harmonic(perm[z, part], halo[0, part] * inside[side])
                diagonal = diagonal + term
                residual = residual + term * (halo[1, part] - pressure[z, part])
                face_z[side, part] = free * term
            for side, tile, row in ((0, 0, 0), (1, rows - ROWS, ROWS - 1)):
                if part.start == tile:
                    term, gain = (jnp.broadcast_to(value[z : z + 1], (ROWS, width)) for value in gain_y[side])
                    diagonal = diagonal + jnp.where(sub == row, term, 0.0)
                    residual = residual + jnp.where(sub == row, gain, 0.0)
            reciprocal = 1.0 / diagonal
            residual = free * residual
            precond = residual * reciprocal
            inverse[z, part] = reciprocal
            u_out[z, part] = residual
            q_out[z, part] = precond
            if part.start == 0:
                y_low[z : z + 1] = precond[:1]
            if part.start == rows - ROWS:
                y_high[z : z + 1] = precond[ROWS - 1 :]

    for z in range(planes):
        plane(z, (0, below_z) if z == 0 else (1, above_z) if z == planes - 1 else None)
    z_low[...] = q_out[0]
    z_high[...] = q_out[planes - 1]
    y_first[...], y_second[...] = to_send(y_low[...], y_high[...])


def apply_planes(q_ref, faces, face_z, face_y, below_z, above_z, y_got, y_got_too, emit, carry):
    planes, rows, width = q_ref.shape
    parts = row_parts(rows)
    below_y, above_y = as_sides(y_got[...], y_got_too[...])
    gain = (face_y[0] * below_y, face_y[1] * above_y)
    sub = lax.broadcasted_iota(jnp.int32, (ROWS, width), 0)
    closed = jnp.zeros((ROWS, width), F32)
    for z in range(planes):
        values = [q_ref[z, part] for part in parts]
        lower, upper = row_shifts(values, closed, closed)
        for at, part in enumerate(parts):
            left, right = lane_shifts(values[at])
            if z == 0:
                u = face_z[0, part] * below_z[part] + faces[1, z, part] * q_ref[z + 1, part]
            elif z == planes - 1:
                u = faces[0, z, part] * q_ref[z - 1, part] + face_z[1, part] * above_z[part]
            else:
                u = faces[0, z, part] * q_ref[z - 1, part] + faces[1, z, part] * q_ref[z + 1, part]
            u = u + faces[2, z, part] * lower[at] + faces[3, z, part] * upper[at]
            u = u + faces[4, z, part] * left + faces[5, z, part] * right
            for side, tile, row in ((0, 0, 0), (1, rows - ROWS, ROWS - 1)):
                if part.start == tile:
                    u = u + jnp.where(sub == row, jnp.broadcast_to(gain[side][z : z + 1], (ROWS, width)), 0.0)
            carry = emit(z, part, u, carry)
    return carry


def stage_kernel(
    q_ref, faces, face_z, face_y, inverse, below_z, above_z, y_got, y_got_too,
    q_out, u_out, z_low, z_high, y_first, y_second,
    y_low, y_high,
):
    planes, rows, _ = q_ref.shape

    def emit(z, part, u, carry):
        q = u * inverse[z, part]
        u_out[z, part] = u
        q_out[z, part] = q
        if z == 0:
            z_low[part] = q
        if z == planes - 1:
            z_high[part] = q
        if part.start == 0:
            y_low[z : z + 1] = q[:1]
        if part.start == rows - ROWS:
            y_high[z : z + 1] = q[ROWS - 1 :]
        return carry

    apply_planes(q_ref, faces, face_z, face_y, below_z, above_z, y_got, y_got_too, emit, 0)
    y_first[...], y_second[...] = to_send(y_low[...], y_high[...])


def fold(product):
    total = product[:, :LANES]
    for at in range(LANES, product.shape[1], LANES):
        total = total + product[:, at : at + LANES]
    return total


def gram_kernel(sums, count, *refs):
    us, qs = refs[: count], refs[count : 2 * count]
    ratio, out = refs[2 * count :]
    planes, rows, _ = ratio.shape

    def body(z, totals):
        totals = list(totals)
        for at in range(0, rows, ROWS):
            part = pl.ds(at, ROWS)
            fields = {("u", i): us[i][z, part] for i in range(count)}
            fields |= {("q", i): qs[i][z, part] for i in range(count)}
            weight = ratio[z, part]
            fields |= {("y", i): weight * fields["q", i] for i in range(count)}
            for number, (a, i, b, j) in enumerate(sums):
                totals[number] = totals[number] + fold(fields[a, i] * fields[b, j])
        return tuple(totals)

    zero = jnp.zeros((ROWS, LANES), F32)
    for number, total in enumerate(lax.fori_loop(0, planes, body, (zero,) * len(sums))):
        out[number] = total


def last_kernel(
    q2_ref, faces, face_z, face_y, u0_ref, u1_ref, u2_ref, below_z, above_z, y_got, y_got_too, early, middle, out
):
    us = (u0_ref, u1_ref, u2_ref)

    def emit(z, part, u3, totals):
        fields = {("u", i): us[i][z, part] for i in range(3)}
        fields |= {("u", 3): u3, ("q", 2): q2_ref[z, part]}
        return [
            total + fold(fields[a, i] * fields[b, j]) for total, (a, i, b, j) in zip(totals, LATE)
        ]

    zero = jnp.zeros((ROWS, LANES), F32)
    late = apply_planes(
        q2_ref, faces, face_z, face_y, below_z, above_z, y_got, y_got_too, emit, [zero] * len(LATE)
    )
    lane = lax.broadcasted_iota(jnp.int32, (1, LANES), 1)
    row = jnp.zeros((1, LANES), F32)
    for names, totals in ((EARLY, early), (MIDDLE, middle), (LATE, late)):
        for number, name in enumerate(names):
            row = jnp.where(lane == SUMS.index(name), jnp.sum(totals[number], keepdims=True), row)
    out[...] = jnp.broadcast_to(row, out.shape)


def quadratic(left, table, right):
    total = None
    for i, a in enumerate(left):
        for j, b in enumerate(right):
            if a is None or b is None:
                continue
            term = a * b * table(i, j)
            total = term if total is None else total + term
    return total


def combine(totals, cell_count, iterations=3):
    moment = lambda i, j: totals[i + j]
    drop = lambda i, j: totals[i + j] - totals[i + j + 1]
    zero = jnp.zeros_like(totals[0])
    one = zero + 1.0
    residual, direction, change = [one], [one], []
    inner = moment(0, 0)
    for step in range(iterations):
        curvature = quadratic(direction, drop, direction)
        alive = (inner > 0.0) & (curvature > 0.0)
        size = jnp.where(alive, inner / jnp.where(alive, curvature, 1.0), 0.0)
        change = [c + size * d for c, d in zip(change + [zero], direction)]
        image = [a - b for a, b in zip(direction + [zero], [zero] + direction)]
        residual = [r - size * a for r, a in zip(residual + [zero], image)]
        if step + 1 < iterations:
            following = quadratic(residual, moment, residual)
            noise = quadratic([abs(r) for r in residual], lambda i, j: abs(moment(i, j)), [abs(r) for r in residual])
            following = jnp.where(following > 1e-7 * noise, following, 0.0)
            growth = jnp.where(inner > 0.0, following / jnp.where(inner > 0.0, inner, 1.0), 0.0)
            direction = [z + growth * d for z, d in zip(residual, direction + [zero])]
            inner = following
    at = {name: total for name, total in zip(SUMS, totals)}
    closing = quadratic(residual, lambda i, j: at["u", min(i, j), "u", max(i, j)], residual)
    changed = quadratic(change, lambda i, j: at["y", min(i, j), "y", max(i, j)], change)
    scale = 1.0 / cell_count
    return change, jnp.sqrt(jnp.maximum(closing, 0.0) * scale), jnp.sqrt(jnp.maximum(changed, 0.0) * scale)


def final_kernel(cell_count, rows_ref, q0, q1, q2, pressure_ref, strain_ref, ratio, pressure_out, strain_out, norms):
    planes, rows, width = pressure_ref.shape
    lane = lax.broadcasted_iota(jnp.int32, (1, LANES), 1)
    row = jnp.sum(rows_ref[...], axis=0, keepdims=True)
    totals = [jnp.sum(jnp.where(lane == at, row, 0.0), axis=1, keepdims=True) for at in range(len(SUMS))]
    change, closing, changed = combine(totals, cell_count)
    norms[...] = jnp.where(lane == 0, closing, changed)[:, :2]
    weights = [jnp.broadcast_to(c, (ROWS, width)) for c in change]

    def body(z, carry):
        for at in range(0, rows, ROWS):
            part = pl.ds(at, ROWS)
            delta = weights[0] * q0[z, part] + weights[1] * q1[z, part] + weights[2] * q2[z, part]
            pressure_out[z, part] = pressure_ref[z, part] + delta
            strain_out[z, part] = strain_ref[z, part] + ratio[z, part] * delta
        return carry

    lax.fori_loop(0, planes, body, 0)


def ring(count, step):
    return [(i, (i + step) % count) for i in range(count)]


def pairs_along_y(count_z, count_y, start):
    pairs = []
    for z in range(count_z):
        partner = list(range(count_y))
        for y in range(start, count_y - 1, 2):
            partner[y], partner[y + 1] = y + 1, y
        pairs += [
            (z * count_y + y, (z if partner[y] != y else z ^ 1) * count_y + partner[y]) for y in range(count_y)
        ]
    return pairs


def exchange(z_low, z_high, y_first, y_second):
    count_z, count_y = lax.axis_size("gz"), lax.axis_size("gy")
    both = ("gz", "gy")
    if paired(count_z, count_y):
        ways = [(both, pairs_along_y(count_z, count_y, start)) for start in (0, 1)]
    else:
        ways = [("gy", ring(count_y, step)) for step in (1, -1)]
    got = {}
    for name, field, axis, pairs in (
        ("send_low", z_low, "gz", ring(count_z, -1)),
        ("send_high", z_high, "gz", ring(count_z, 1)),
        ("send_first", y_first, *ways[0]),
        ("send_second", y_second, *ways[1]),
    ):
        got[name] = lax.ppermute(field, axis, pairs)
    return got["send_high"], got["send_low"], got["send_first"], got["send_second"]


def call(kernel, outs, specs, *operands, scratch=(), keep=True):
    shapes = [pltpu.VMEM(shape, F32) if keep else jax.ShapeDtypeStruct(shape, F32) for shape in outs]
    operands = [
        pltpu.with_memory_space_constraint(operand, spec.memory_space) for operand, spec in zip(operands, specs)
    ]
    single = len(shapes) == 1
    return pl.pallas_call(
        kernel,
        out_shape=shapes[0] if single else shapes,
        in_specs=specs,
        out_specs=VMEM if single else [VMEM] * len(shapes),
        scratch_shapes=list(scratch),
        compiler_params=pltpu.CompilerParams(vmem_limit_bytes=16 << 20),
    )(*operands)


def per_device(
    zone_ids, fixed_cells, pressure_old, pressure_iter, strain_change, source,
    zone_perm, zone_storage, zone_biot, zone_bulk,
):
    planes, rows, width = zone_ids.shape
    field = (planes, rows, width)
    sides = ((rows, width), (rows, width), (planes, width), (planes, width))
    devices = lax.axis_size("gz") * lax.axis_size("gy")
    cell_count = zone_ids.size * devices
    line = pltpu.VMEM((planes, width), F32)

    packed = call(
        pack_kernel, [(2, *side) for side in sides], [HBM] * 3, zone_ids, pressure_iter, zone_perm,
        scratch=[
            pltpu.VMEM((2, rows, width), jnp.int32), pltpu.VMEM((2, planes, ROWS, width), jnp.int32),
            pltpu.VMEM((2, planes, ROWS, width), F32), pltpu.SMEM(zone_perm.shape, F32), pltpu.SemaphoreType.DMA((9,)),
        ],
    )
    halo = exchange(*packed)
    faces, perm, diagonal, residual, free, ratio, pressure_kept, strain_kept = call(
        prepare_kernel, [(6, *field)] + [field] * 7, [HBM] * 10,
        zone_ids, fixed_cells, pressure_old, pressure_iter, strain_change, source,
        zone_perm, zone_storage, zone_biot, zone_bulk,
        scratch=[
            *[pltpu.VMEM(field, jnp.int32)] * 2, *[pltpu.VMEM(field, F32)] * 2,
            *[pltpu.SMEM(zone_perm.shape, F32)] * 4, pltpu.SemaphoreType.DMA((10,)),
        ],
    )
    inverse, q0, u0, face_z, face_y, *edges = call(
        begin_kernel, [field, field, field, (2, rows, width), (2, planes, width), *sides], [VMEM] * 9,
        perm, diagonal, residual, free, pressure_kept, *halo, scratch=[line, line],
    )
    parts = (faces, face_z, face_y)
    halo = exchange(*edges)
    q1, u1, *edges = call(
        stage_kernel, [field, field, *sides], [VMEM] * 9, q0, *parts, inverse, *halo, scratch=[line, line]
    )
    halo = exchange(*edges)
    early = call(
        functools.partial(gram_kernel, EARLY, 2), [(len(EARLY), ROWS, LANES)], [VMEM] * 5,
        u0, u1, q0, q1, ratio,
    )
    q2, u2, *edges = call(
        stage_kernel, [field, field, *sides], [VMEM] * 9, q1, *parts, inverse, *halo, scratch=[line, line]
    )
    halo = exchange(*edges)
    middle = call(
        functools.partial(gram_kernel, MIDDLE, 3), [(len(MIDDLE), ROWS, LANES)], [VMEM] * 7,
        u0, u1, u2, q0, q1, q2, ratio,
    )
    sums = call(
        last_kernel, [(devices, LANES)], [VMEM] * 13,
        q2, *parts, u0, u1, u2, *halo, early, middle,
    )
    gathered = lax.all_to_all(sums, ("gz", "gy"), 0, 0, tiled=True)
    pressure, strain_next, norms = call(
        functools.partial(final_kernel, cell_count), [field, field, (1, 2)], [VMEM] * 7,
        gathered, q0, q1, q2, pressure_kept, strain_kept, ratio, keep=False,
    )
    return pressure, strain_next, norms.reshape(2)


def solution(mesh):
    split = P("gz", "gy", None)
    return jax.shard_map(
        per_device,
        mesh=mesh,
        in_specs=(split,) * 6 + (P(),) * 4,
        out_specs=(split, split, P()),
        check_vma=False,
    )
```

```python
import functools

import jax
import jax.numpy as jnp
from jax import lax
from jax.experimental import pallas as pl
from jax.experimental.pallas import tpu as pltpu
from jax.sharding import PartitionSpec as P

F32 = jnp.float32
ROWS = 8
LANES = 128
VMEM = pl.BlockSpec(memory_space=pltpu.VMEM)
HBM = pl.BlockSpec(memory_space=pltpu.HBM)

MOMENTS = (("q", 0, "u", 0), ("q", 0, "u", 1), ("q", 1, "u", 1), ("q", 1, "u", 2), ("q", 2, "u", 2), ("q", 2, "u", 3))
CLOSING = tuple(("u", i, "u", j) for i in range(4) for j in range(i, 4))
CHANGE = tuple(("y", i, "y", j) for i in range(3) for j in range(i, 3))
SUMS = MOMENTS + CLOSING + CHANGE
EARLY = tuple(s for s in SUMS if max(s[1], s[3]) <= 1)
MIDDLE = tuple(s for s in SUMS if max(s[1], s[3]) == 2)
LATE = tuple(s for s in SUMS if max(s[1], s[3]) == 3)


def table_row(table_ref):
    lane = lax.broadcasted_iota(jnp.int32, (ROWS, LANES), 1)
    row = jnp.zeros((ROWS, LANES), F32)
    for zone in range(table_ref.shape[0]):
        row = jnp.where(lane == zone, table_ref[zone], row)
    return row


def look_up(row, zones):
    parts = [
        jnp.take_along_axis(row, zones[:, at : at + LANES], axis=1, mode="promise_in_bounds")
        for at in range(0, zones.shape[1], LANES)
    ]
    return jnp.concatenate(parts, axis=1)


def zone_bits(zones, count):
    return [(zones & (1 << bit)) != 0 for bit in range(max(count - 1, 1).bit_length())]


def pick(bits, entries):
    entries = list(entries) + [entries[-1]] * (2 ** len(bits) - len(entries))
    for bit in bits:
        entries = [jnp.where(bit, odd, even) for even, odd in zip(entries[::2], entries[1::2])]
    return entries[0]


def harmonic(lower_side, upper_side):
    return 2.0 * lower_side * upper_side / (lower_side + upper_side)


def row_shifts(tiles, before, after):
    sub = lax.broadcasted_iota(jnp.int32, tiles[0].shape, 0)
    down = [pltpu.roll(tile, 1, 0) for tile in tiles]
    up = [pltpu.roll(tile, ROWS - 1, 0) for tile in tiles]
    lower, upper = [], []
    for at in range(len(tiles)):
        lower.append(jnp.where(sub == 0, down[at - 1] if at else before, down[at]))
        upper.append(jnp.where(sub == ROWS - 1, up[at + 1] if at + 1 < len(tiles) else after, up[at]))
    return lower, upper


def lane_shifts(tile):
    width = tile.shape[1]
    return pltpu.roll(tile, 1, 1), pltpu.roll(tile, width - 1, 1)


def paired(count_z, count_y):
    return count_z % 2 == 0 and count_y % 2 == 0


def to_send(low, high):
    if not paired(lax.axis_size("gz"), lax.axis_size("gy")):
        return high, low
    odd = lax.rem(lax.axis_index("gy"), 2) == 1
    return jnp.where(odd, low, high), jnp.where(odd, high, low)


def as_sides(first, second):
    if not paired(lax.axis_size("gz"), lax.axis_size("gy")):
        return first, second
    odd = lax.rem(lax.axis_index("gy"), 2) == 1
    return jnp.where(odd, first, second), jnp.where(odd, second, first)


def inside_flags():
    flags = []
    for axis in ("gz", "gy"):
        place = lax.axis_index(axis)
        flags += [place > 0, place < lax.axis_size(axis) - 1]
    return flags


def row_parts(rows):
    return [pl.ds(at, ROWS) for at in range(0, rows, ROWS)]


def pack_kernel(
    zone_hbm, pressure_hbm, z_low, z_high, y_first, y_second, zone_z, zone_y, pressure_y, sems
):
    planes, rows, _ = zone_hbm.shape
    ends = ((0, pl.ds(0, ROWS)), (planes - 1, pl.ds(rows - ROWS, ROWS)))
    copies = []
    for side, (plane, part) in enumerate(ends):
        out = (z_low, z_high)[side]
        for source, target in (
            (zone_hbm.at[plane], zone_z.at[side]),
            (pressure_hbm.at[plane], out.at[1]),
            (zone_hbm.at[:, part], zone_y.at[side]),
            (pressure_hbm.at[:, part], pressure_y.at[side]),
        ):
            copies.append(pltpu.make_async_copy(source, target, sems.at[len(copies)]))
    for copy in copies:
        copy.start()
    for copy in copies:
        copy.wait()
    faces_y = []
    for side, out in enumerate((z_low, z_high)):
        out[0] = zone_z[side].astype(F32)
        row = pl.ds((0, ROWS - 1)[side], 1)
        zones = jnp.concatenate([zone_y[side, plane, row] for plane in range(planes)], axis=0)
        values = jnp.concatenate([pressure_y[side, plane, row] for plane in range(planes)], axis=0)
        faces_y.append((zones.astype(F32), values))
    for number in range(2):
        y_first[number], y_second[number] = to_send(faces_y[0][number], faces_y[1][number])


NO_FACE = LANES - 1


def face_row(perm_row, zones):
    lane = lax.broadcasted_iota(jnp.int32, (ROWS, LANES), 1)
    known = lane < zones * zones
    pair = jnp.where(known, lane, 0)
    sides = [
        jnp.take_along_axis(perm_row, side, axis=1, mode="promise_in_bounds")
        for side in (lax.div(pair, zones), lax.rem(pair, zones))
    ]
    return jnp.where(known, harmonic(*sides), 0.0)


def prepare_kernel(
    zone_hbm, fixed_hbm, old_hbm, pressure_hbm, strain_hbm, source_hbm,
    perm_hbm, storage_hbm, biot_hbm, bulk_hbm,
    faces, diagonal_out, residual_out, free_out, ratio, pressure, strain, face_table, zone,
    fixed, old, source, perm, storage_of, biot_of, term_z, perm_table, storage_table, biot_table, bulk_table, sems, half_sems,
):
    planes, rows, width = zone_hbm.shape
    half = planes // 2
    pairs = (
        (zone_hbm, zone), (perm_hbm, perm_table), (storage_hbm, storage_table), (biot_hbm, biot_table),
        (bulk_hbm, bulk_table), (pressure_hbm, pressure),
    )
    copies = [pltpu.make_async_copy(*pair, sems.at[number]) for number, pair in enumerate(pairs)]
    halves = [
        [
            pltpu.make_async_copy(whole.at[part], kept.at[part], half_sems.at[at, number])
            for number, (whole, kept) in enumerate(
                ((fixed_hbm, fixed), (old_hbm, old), (strain_hbm, strain), (source_hbm, source))
            )
        ]
        for at, part in enumerate((pl.ds(0, half), pl.ds(half, planes - half)))
    ]
    for copy in copies + halves[0] + halves[1]:
        copy.start()
    for copy in copies[1:5]:
        copy.wait()
    zones = perm_table.shape[0]
    face_table[...] = face_row(table_row(perm_table), zones)
    entries = [[table[number] for number in range(zones)] for table in (perm_table, storage_table, biot_table)]
    one = jnp.ones((ROWS, width), F32)
    entries.append([entries[2][number] * one / (bulk_table[number] * one) for number in range(zones)])
    lane = lax.broadcasted_iota(jnp.int32, (ROWS, width), 1)
    closed = jnp.zeros((ROWS, width), F32)
    parts = row_parts(rows)
    copies[0].wait()

    def fill(z, carry):
        for part in parts:
            bits = zone_bits(zone[z, part], zones)
            for out, entry in zip((perm, storage_of, biot_of, ratio), entries):
                out[z, part] = pick(bits, entry)
        return carry

    lax.fori_loop(0, planes, fill, 0)
    copies[5].wait()

    def plane(z, low, high):
        perms = [perm[z, part] for part in parts]
        values = [pressure[z, part] for part in parts]
        perm_lower, _ = row_shifts(perms, closed, closed)
        lower = [harmonic(*pair) for pair in zip(perms, perm_lower)]
        _, upper = row_shifts(lower, closed, closed)
        value_lower, value_upper = row_shifts(values, closed, closed)
        for at, part in enumerate(parts):
            here, value = perms[at], values[at]
            left = harmonic(here, jnp.where(lane == 0, 0.0, pltpu.roll(here, 1, 1)))
            right = pltpu.roll(left, width - 1, 1)
            terms, views = [None, None], [None, None]
            if low is not None:
                terms[0], views[0] = term_z[z, part], pressure[low, part]
            if high is not None:
                terms[1], views[1] = harmonic(here, perm[high, part]), pressure[high, part]
                term_z[high, part] = terms[1]
            terms += [lower[at], upper[at], left, right]
            views += [value_lower[at], value_upper[at], *lane_shifts(value)]
            storage, biot = storage_of[z, part], biot_of[z, part]
            coupling = biot * ratio[z, part]
            free = 1.0 - fixed[z, part].astype(F32)
            diagonal, neighbours = storage + coupling, None
            for number, (term, view) in enumerate(zip(terms, views)):
                if term is not None:
                    faces[number, z, part] = free * term
                    diagonal = diagonal + term
                    neighbours = term * view if neighbours is None else neighbours + term * view
            right_side = storage * old[z, part] + coupling * value - biot * strain[z, part] + source[z, part]
            diagonal_out[z, part] = diagonal
            residual_out[z, part] = right_side - (diagonal * value - neighbours)
            free_out[z, part] = free

    def middle(start, stop):
        lax.fori_loop(start, stop, lambda z, c: (plane(z, z - 1, z + 1), c)[1], 0)

    for copy in halves[0]:
        copy.wait()
    plane(0, None, 1)
    middle(1, half)
    for copy in halves[1]:
        copy.wait()
    middle(half, planes - 1)
    plane(planes - 1, planes - 2, None)


def begin_kernel(
    zones,
    zone, face_table, diagonal_ref, residual_ref, free_ref, pressure, below_z, above_z, y_got, y_got_too,
    inverse, q_out, u_out, face_z, face_y, z_low, z_high, y_first, y_second,
    y_low, y_high,
):
    planes, rows, width = pressure.shape
    inside = inside_flags()
    below_zone, above_zone = as_sides(y_got[0], y_got_too[0])
    below_value, above_value = as_sides(y_got[1], y_got_too[1])
    table = face_table[...]

    def outer_term(own, other, side):
        index = own * zones + other.astype(jnp.int32)
        return look_up(table, jnp.where(inside[side], index, NO_FACE))

    sub = lax.broadcasted_iota(jnp.int32, (ROWS, width), 0)
    ends = (
        (pl.ds(0, 1), below_zone, below_value),
        (pl.ds(rows - 1, 1), above_zone, above_value),
    )
    gain_y = []
    for side, (row, other, value) in enumerate(ends):
        here = jnp.concatenate([zone[z, row] for z in range(planes)], axis=0)
        own = jnp.concatenate([pressure[z, row] for z in range(planes)], axis=0)
        free = jnp.concatenate([free_ref[z, row] for z in range(planes)], axis=0)
        term = outer_term(here, other, 2 + side)
        face_y[side] = free * term
        gain_y.append((term, term * (value - own)))

    def plane(z, outer):
        for part in row_parts(rows):
            diagonal, residual, free = diagonal_ref[z, part], residual_ref[z, part], free_ref[z, part]
            if outer is not None:
                side, halo = outer
                term = outer_term(zone[z, part], halo[0, part], side)
                diagonal = diagonal + term
                residual = residual + term * (halo[1, part] - pressure[z, part])
                face_z[side, part] = free * term
            for side, tile, row in ((0, 0, 0), (1, rows - ROWS, ROWS - 1)):
                if part.start == tile:
                    term, gain = (jnp.broadcast_to(value[z : z + 1], (ROWS, width)) for value in gain_y[side])
                    diagonal = diagonal + jnp.where(sub == row, term, 0.0)
                    residual = residual + jnp.where(sub == row, gain, 0.0)
            reciprocal = 1.0 / diagonal
            residual = free * residual
            precond = residual * reciprocal
            inverse[z, part] = reciprocal
            u_out[z, part] = residual
            q_out[z, part] = precond
            if part.start == 0:
                y_low[z : z + 1] = precond[:1]
            if part.start == rows - ROWS:
                y_high[z : z + 1] = precond[ROWS - 1 :]

    for z in range(planes):
        plane(z, (0, below_z) if z == 0 else (1, above_z) if z == planes - 1 else None)
    z_low[...] = q_out[0]
    z_high[...] = q_out[planes - 1]
    y_first[...], y_second[...] = to_send(y_low[...], y_high[...])


def apply_planes(q_ref, faces, face_z, face_y, below_z, above_z, y_got, y_got_too, emit, carry):
    planes, rows, width = q_ref.shape
    parts = row_parts(rows)
    below_y, above_y = as_sides(y_got[...], y_got_too[...])
    gain = (face_y[0] * below_y, face_y[1] * above_y)
    sub = lax.broadcasted_iota(jnp.int32, (ROWS, width), 0)
    closed = jnp.zeros((ROWS, width), F32)
    for z in range(planes):
        values = [q_ref[z, part] for part in parts]
        lower, upper = row_shifts(values, closed, closed)
        for at, part in enumerate(parts):
            left, right = lane_shifts(values[at])
            if z == 0:
                u = face_z[0, part] * below_z[part] + faces[1, z, part] * q_ref[z + 1, part]
            elif z == planes - 1:
                u = faces[0, z, part] * q_ref[z - 1, part] + face_z[1, part] * above_z[part]
            else:
                u = faces[0, z, part] * q_ref[z - 1, part] + faces[1, z, part] * q_ref[z + 1, part]
            u = u + faces[2, z, part] * lower[at] + faces[3, z, part] * upper[at]
            u = u + faces[4, z, part] * left + faces[5, z, part] * right
            for side, tile, row in ((0, 0, 0), (1, rows - ROWS, ROWS - 1)):
                if part.start == tile:
                    u = u + jnp.where(sub == row, jnp.broadcast_to(gain[side][z : z + 1], (ROWS, width)), 0.0)
            carry = emit(z, part, u, carry)
    return carry


def stage_kernel(
    q_ref, faces, face_z, face_y, inverse, below_z, above_z, y_got, y_got_too,
    q_out, u_out, z_low, z_high, y_first, y_second,
    y_low, y_high,
):
    planes, rows, _ = q_ref.shape

    def emit(z, part, u, carry):
        q = u * inverse[z, part]
        u_out[z, part] = u
        q_out[z, part] = q
        if z == 0:
            z_low[part] = q
        if z == planes - 1:
            z_high[part] = q
        if part.start == 0:
            y_low[z : z + 1] = q[:1]
        if part.start == rows - ROWS:
            y_high[z : z + 1] = q[ROWS - 1 :]
        return carry

    apply_planes(q_ref, faces, face_z, face_y, below_z, above_z, y_got, y_got_too, emit, 0)
    y_first[...], y_second[...] = to_send(y_low[...], y_high[...])


def fold(product):
    total = product[:, :LANES]
    for at in range(LANES, product.shape[1], LANES):
        total = total + product[:, at : at + LANES]
    return total


def gram_kernel(sums, count, *refs):
    us, qs = refs[: count], refs[count : 2 * count]
    ratio, out = refs[2 * count :]
    planes, rows, _ = ratio.shape

    def body(z, totals):
        totals = list(totals)
        for at in range(0, rows, ROWS):
            part = pl.ds(at, ROWS)
            fields = {("u", i): us[i][z, part] for i in range(count)}
            fields |= {("q", i): qs[i][z, part] for i in range(count)}
            weight = ratio[z, part]
            fields |= {("y", i): weight * fields["q", i] for i in range(count)}
            for number, (a, i, b, j) in enumerate(sums):
                totals[number] = totals[number] + fold(fields[a, i] * fields[b, j])
        return tuple(totals)

    zero = jnp.zeros((ROWS, LANES), F32)
    for number, total in enumerate(lax.fori_loop(0, planes, body, (zero,) * len(sums))):
        out[number] = total


def last_kernel(
    q2_ref, faces, face_z, face_y, u0_ref, u1_ref, u2_ref, below_z, above_z, y_got, y_got_too, early, middle, out
):
    us = (u0_ref, u1_ref, u2_ref)

    def emit(z, part, u3, totals):
        fields = {("u", i): us[i][z, part] for i in range(3)}
        fields |= {("u", 3): u3, ("q", 2): q2_ref[z, part]}
        return [
            total + fold(fields[a, i] * fields[b, j]) for total, (a, i, b, j) in zip(totals, LATE)
        ]

    zero = jnp.zeros((ROWS, LANES), F32)
    late = apply_planes(
        q2_ref, faces, face_z, face_y, below_z, above_z, y_got, y_got_too, emit, [zero] * len(LATE)
    )
    lane = lax.broadcasted_iota(jnp.int32, (1, LANES), 1)
    row = jnp.zeros((1, LANES), F32)
    for names, totals in ((EARLY, early), (MIDDLE, middle), (LATE, late)):
        for number, name in enumerate(names):
            row = jnp.where(lane == SUMS.index(name), jnp.sum(totals[number], keepdims=True), row)
    out[...] = jnp.broadcast_to(row, out.shape)


def quadratic(left, table, right):
    total = None
    for i, a in enumerate(left):
        for j, b in enumerate(right):
            if a is None or b is None:
                continue
            term = a * b * table(i, j)
            total = term if total is None else total + term
    return total


def combine(totals, cell_count, iterations=3):
    moment = lambda i, j: totals[i + j]
    drop = lambda i, j: totals[i + j] - totals[i + j + 1]
    zero = jnp.zeros_like(totals[0])
    one = zero + 1.0
    residual, direction, change = [one], [one], []
    inner = moment(0, 0)
    for step in range(iterations):
        curvature = quadratic(direction, drop, direction)
        alive = (inner > 0.0) & (curvature > 0.0)
        size = jnp.where(alive, inner / jnp.where(alive, curvature, 1.0), 0.0)
        change = [c + size * d for c, d in zip(change + [zero], direction)]
        image = [a - b for a, b in zip(direction + [zero], [zero] + direction)]
        residual = [r - size * a for r, a in zip(residual + [zero], image)]
        if step + 1 < iterations:
            following = quadratic(residual, moment, residual)
            noise = quadratic([abs(r) for r in residual], lambda i, j: abs(moment(i, j)), [abs(r) for r in residual])
            following = jnp.where(following > 1e-7 * noise, following, 0.0)
            growth = jnp.where(inner > 0.0, following / jnp.where(inner > 0.0, inner, 1.0), 0.0)
            direction = [z + growth * d for z, d in zip(residual, direction + [zero])]
            inner = following
    at = {name: total for name, total in zip(SUMS, totals)}
    closing = quadratic(residual, lambda i, j: at["u", min(i, j), "u", max(i, j)], residual)
    changed = quadratic(change, lambda i, j: at["y", min(i, j), "y", max(i, j)], change)
    scale = 1.0 / cell_count
    return change, jnp.sqrt(jnp.maximum(closing, 0.0) * scale), jnp.sqrt(jnp.maximum(changed, 0.0) * scale)


def final_kernel(
    cell_count, rows_ref, q0, q1, q2, pressure_ref, strain_ref, ratio, pressure_hbm, strain_hbm, norms_hbm,
    pressure_out, strain_out, norms, sems, norms_sem,
):
    planes, rows, width = pressure_ref.shape
    total = rows_ref[:ROWS]
    for at in range(ROWS, rows_ref.shape[0], ROWS):
        total = total + rows_ref[at : at + ROWS]
    for step in (4, 2, 1):
        total = total + pltpu.roll(total, step, 0)
    totals = [
        jnp.take_along_axis(total, jnp.full((ROWS, LANES), at, jnp.int32), axis=1, mode="promise_in_bounds")
        for at in range(len(SUMS))
    ]
    change, closing, changed = combine(totals, cell_count)
    lane = lax.broadcasted_iota(jnp.int32, (1, LANES), 1)
    norms[...] = jnp.where(lane == 0, closing[:1], changed[:1])[:, :2]
    norms_copy = pltpu.make_async_copy(norms, norms_hbm, norms_sem)
    norms_copy.start()
    weights = [jnp.concatenate([c] * (width // LANES), axis=1) for c in change]

    def copies(z):
        return [
            pltpu.make_async_copy(kept.at[z], whole.at[z], sems.at[number, z])
            for number, (kept, whole) in enumerate(((pressure_out, pressure_hbm), (strain_out, strain_hbm)))
        ]

    for z in range(planes):
        for part in row_parts(rows):
            delta = weights[0] * q0[z, part] + weights[1] * q1[z, part] + weights[2] * q2[z, part]
            pressure_out[z, part] = pressure_ref[z, part] + delta
            strain_out[z, part] = strain_ref[z, part] + ratio[z, part] * delta
        for copy in copies(z):
            copy.start()
    for z in range(planes):
        for copy in copies(z):
            copy.wait()
    norms_copy.wait()


def ring(count, step):
    return [(i, (i + step) % count) for i in range(count)]


def pairs_along_y(count_z, count_y, start):
    pairs = []
    for z in range(count_z):
        partner = list(range(count_y))
        for y in range(start, count_y - 1, 2):
            partner[y], partner[y + 1] = y + 1, y
        pairs += [
            (z * count_y + y, (z if partner[y] != y else z ^ 1) * count_y + partner[y]) for y in range(count_y)
        ]
    return pairs


def exchange(z_low, z_high, y_first, y_second):
    count_z, count_y = lax.axis_size("gz"), lax.axis_size("gy")
    both = ("gz", "gy")
    if paired(count_z, count_y):
        ways = [(both, pairs_along_y(count_z, count_y, start)) for start in (0, 1)]
    else:
        ways = [("gy", ring(count_y, step)) for step in (1, -1)]
    got = {}
    for name, field, axis, pairs in (
        ("send_low", z_low, "gz", ring(count_z, -1)),
        ("send_high", z_high, "gz", ring(count_z, 1)),
        ("send_first", y_first, *ways[0]),
        ("send_second", y_second, *ways[1]),
    ):
        got[name] = lax.ppermute(field, axis, pairs)
    return got["send_high"], got["send_low"], got["send_first"], got["send_second"]


def call(kernel, outs, specs, *operands, scratch=(), out_specs=None):
    results = [pltpu.VMEM(out, F32) if isinstance(out, tuple) else out for out in outs]
    out_specs = out_specs or [VMEM] * len(results)
    operands = [
        pltpu.with_memory_space_constraint(operand, spec.memory_space) for operand, spec in zip(operands, specs)
    ]
    single = len(results) == 1
    return pl.pallas_call(
        kernel,
        out_shape=results[0] if single else results,
        in_specs=specs,
        out_specs=out_specs[0] if single else out_specs,
        scratch_shapes=list(scratch),
        compiler_params=pltpu.CompilerParams(vmem_limit_bytes=16 << 20),
    )(*operands)


def per_device(
    zone_ids, fixed_cells, pressure_old, pressure_iter, strain_change, source,
    zone_perm, zone_storage, zone_biot, zone_bulk,
):
    planes, rows, width = zone_ids.shape
    field = (planes, rows, width)
    sides = ((rows, width), (rows, width), (planes, width), (planes, width))
    devices = lax.axis_size("gz") * lax.axis_size("gy")
    cell_count = zone_ids.size * devices
    line = pltpu.VMEM((planes, width), F32)

    packed = call(
        pack_kernel, [(2, *side) for side in sides], [HBM] * 2, zone_ids, pressure_iter,
        scratch=[
            pltpu.VMEM((2, rows, width), jnp.int32), pltpu.VMEM((2, planes, ROWS, width), jnp.int32),
            pltpu.VMEM((2, planes, ROWS, width), F32), pltpu.SemaphoreType.DMA((8,)),
        ],
    )
    halo = exchange(*packed)
    faces, diagonal, residual, free, ratio, pressure_kept, strain_kept, face_table, zone_kept = call(
        prepare_kernel,
        [(6, *field)] + [field] * 6 + [(ROWS, LANES), pltpu.VMEM(field, jnp.int32)], [HBM] * 10,
        zone_ids, fixed_cells, pressure_old, pressure_iter, strain_change, source,
        zone_perm, zone_storage, zone_biot, zone_bulk,
        scratch=[
            pltpu.VMEM(field, jnp.int32), *[pltpu.VMEM(field, F32)] * 6, *[pltpu.SMEM(zone_perm.shape, F32)] * 4,
            pltpu.SemaphoreType.DMA((6,)), pltpu.SemaphoreType.DMA((2, 4)),
        ],
    )
    inverse, q0, u0, face_z, face_y, *edges = call(
        functools.partial(begin_kernel, zone_perm.shape[0]),
        [field, field, field, (2, rows, width), (2, planes, width), *sides], [VMEM] * 10,
        zone_kept, face_table, diagonal, residual, free, pressure_kept, *halo, scratch=[line, line],
    )
    parts = (faces, face_z, face_y)
    halo = exchange(*edges)
    q1, u1, *edges = call(
        stage_kernel, [field, field, *sides], [VMEM] * 9, q0, *parts, inverse, *halo, scratch=[line, line]
    )
    halo = exchange(*edges)
    early = call(
        functools.partial(gram_kernel, EARLY, 2), [(len(EARLY), ROWS, LANES)], [VMEM] * 5,
        u0, u1, q0, q1, ratio,
    )
    q2, u2, *edges = call(
        stage_kernel, [field, field, *sides], [VMEM] * 9, q1, *parts, inverse, *halo, scratch=[line, line]
    )
    halo = exchange(*edges)
    middle = call(
        functools.partial(gram_kernel, MIDDLE, 3), [(len(MIDDLE), ROWS, LANES)], [VMEM] * 7,
        u0, u1, u2, q0, q1, q2, ratio,
    )
    sums = call(
        last_kernel, [(devices, LANES)], [VMEM] * 13,
        q2, *parts, u0, u1, u2, *halo, early, middle,
    )
    gathered = lax.all_to_all(sums, ("gz", "gy"), 0, 0, tiled=True)
    pressure, strain_next, norms = call(
        functools.partial(final_kernel, cell_count),
        [jax.ShapeDtypeStruct(shape, F32) for shape in (field, field, (1, 2))], [VMEM] * 7,
        gathered, q0, q1, q2, pressure_kept, strain_kept, ratio, out_specs=[HBM] * 3,
        scratch=[
            *[pltpu.VMEM(field, F32)] * 2, pltpu.VMEM((1, 2), F32), pltpu.SemaphoreType.DMA((2, planes)),
            pltpu.SemaphoreType.DMA,
        ],
    )
    return pressure, strain_next, norms.reshape(2)


def solution(mesh):
    split = P("gz", "gy", None)
    return jax.shard_map(
        per_device,
        mesh=mesh,
        in_specs=(split,) * 6 + (P(),) * 4,
        out_specs=(split, split, P()),
        check_vma=False,
    )
```

```python
import functools

import jax
import jax.numpy as jnp
from jax import lax
from jax.experimental import pallas as pl
from jax.experimental.pallas import tpu as pltpu
from jax.sharding import PartitionSpec as P

F32 = jnp.float32
ROWS = 8
LANES = 128
VMEM = pl.BlockSpec(memory_space=pltpu.VMEM)
HBM = pl.BlockSpec(memory_space=pltpu.HBM)

MOMENTS = (("q", 0, "u", 0), ("q", 0, "u", 1), ("q", 1, "u", 1), ("q", 1, "u", 2), ("q", 2, "u", 2), ("q", 2, "u", 3))
CLOSING = tuple(("u", i, "u", j) for i in range(4) for j in range(i, 4))
CHANGE = tuple(("y", i, "y", j) for i in range(3) for j in range(i, 3))
SUMS = MOMENTS + CLOSING + CHANGE
EARLY = tuple(s for s in SUMS if max(s[1], s[3]) <= 1)
MIDDLE = tuple(s for s in SUMS if max(s[1], s[3]) == 2)
LATE = tuple(s for s in SUMS if max(s[1], s[3]) == 3)


def table_row(table_ref):
    lane = lax.broadcasted_iota(jnp.int32, (ROWS, LANES), 1)
    row = jnp.zeros((ROWS, LANES), F32)
    for zone in range(table_ref.shape[0]):
        row = jnp.where(lane == zone, table_ref[zone], row)
    return row


def look_up(row, zones):
    parts = [
        jnp.take_along_axis(row, zones[:, at : at + LANES], axis=1, mode="promise_in_bounds")
        for at in range(0, zones.shape[1], LANES)
    ]
    return jnp.concatenate(parts, axis=1)


def zone_bits(zones, count):
    return [(zones & (1 << bit)) != 0 for bit in range(max(count - 1, 1).bit_length())]


def pick(bits, entries):
    entries = list(entries) + [entries[-1]] * (2 ** len(bits) - len(entries))
    for bit in bits:
        entries = [jnp.where(bit, odd, even) for even, odd in zip(entries[::2], entries[1::2])]
    return entries[0]


def harmonic(lower_side, upper_side):
    return 2.0 * lower_side * upper_side / (lower_side + upper_side)


def row_shifts(tiles, before, after):
    sub = lax.broadcasted_iota(jnp.int32, tiles[0].shape, 0)
    down = [pltpu.roll(tile, 1, 0) for tile in tiles]
    up = [pltpu.roll(tile, ROWS - 1, 0) for tile in tiles]
    lower, upper = [], []
    for at in range(len(tiles)):
        lower.append(jnp.where(sub == 0, down[at - 1] if at else before, down[at]))
        upper.append(jnp.where(sub == ROWS - 1, up[at + 1] if at + 1 < len(tiles) else after, up[at]))
    return lower, upper


def lane_shifts(tile):
    width = tile.shape[1]
    return pltpu.roll(tile, 1, 1), pltpu.roll(tile, width - 1, 1)


def paired(count_z, count_y):
    return count_z % 2 == 0 and count_y % 2 == 0


def to_send(low, high):
    if not paired(lax.axis_size("gz"), lax.axis_size("gy")):
        return high, low
    odd = lax.rem(lax.axis_index("gy"), 2) == 1
    return jnp.where(odd, low, high), jnp.where(odd, high, low)


def as_sides(first, second):
    if not paired(lax.axis_size("gz"), lax.axis_size("gy")):
        return first, second
    odd = lax.rem(lax.axis_index("gy"), 2) == 1
    return jnp.where(odd, first, second), jnp.where(odd, second, first)


def inside_flags():
    flags = []
    for axis in ("gz", "gy"):
        place = lax.axis_index(axis)
        flags += [place > 0, place < lax.axis_size(axis) - 1]
    return flags


def row_parts(rows):
    return [pl.ds(at, ROWS) for at in range(0, rows, ROWS)]


NO_FACE = LANES - 1


def face_row(perm_row, zones):
    lane = lax.broadcasted_iota(jnp.int32, (ROWS, LANES), 1)
    known = lane < zones * zones
    pair = jnp.where(known, lane, 0)
    sides = [
        jnp.take_along_axis(perm_row, side, axis=1, mode="promise_in_bounds")
        for side in (lax.div(pair, zones), lax.rem(pair, zones))
    ]
    return jnp.where(known, harmonic(*sides), 0.0)


def load_kernel(
    zone_hbm, pressure_hbm, fixed_hbm, old_hbm, strain_hbm, source_hbm, perm_hbm, storage_hbm, biot_hbm, bulk_hbm,
    zone, pressure, fixed, old, strain, source, perm, storage, biot, ratio, face_table,
    z_low, z_high, y_first, y_second,
    perm_table, storage_table, biot_table, bulk_table, sems,
):
    planes, rows, width = zone.shape
    pairs = (
        (perm_hbm, perm_table), (storage_hbm, storage_table), (biot_hbm, biot_table), (bulk_hbm, bulk_table),
        (zone_hbm, zone), (pressure_hbm, pressure),
        (fixed_hbm, fixed), (old_hbm, old), (strain_hbm, strain), (source_hbm, source),
    )
    copies = [pltpu.make_async_copy(*pair, sems.at[number]) for number, pair in enumerate(pairs)]
    for copy in copies:
        copy.start()
    for copy in copies[:4]:
        copy.wait()
    zones = perm_table.shape[0]
    face_table[...] = face_row(table_row(perm_table), zones)
    entries = [[table[number] for number in range(zones)] for table in (perm_table, storage_table, biot_table)]
    one = jnp.ones((ROWS, width), F32)
    entries.append([entries[2][number] * one / (bulk_table[number] * one) for number in range(zones)])
    copies[4].wait()

    def fill(z, carry):
        for part in row_parts(rows):
            bits = zone_bits(zone[z, part], zones)
            for out, entry in zip((perm, storage, biot, ratio), entries):
                out[z, part] = pick(bits, entry)
        return carry

    lax.fori_loop(0, planes, fill, 0)
    copies[5].wait()
    faces_y = []
    for side, out in enumerate((z_low, z_high)):
        plane = (0, planes - 1)[side]
        out[0] = zone[plane].astype(F32)
        out[1] = pressure[plane]
        row = pl.ds((0, rows - 1)[side], 1)
        ids = jnp.concatenate([zone[z, row] for z in range(planes)], axis=0)
        values = jnp.concatenate([pressure[z, row] for z in range(planes)], axis=0)
        faces_y.append((ids.astype(F32), values))
    for number in range(2):
        y_first[number], y_second[number] = to_send(faces_y[0][number], faces_y[1][number])
    for copy in copies[6:]:
        copy.wait()


def prepare_kernel(
    pressure, fixed, old, strain, source, perm, storage_of, biot_of, ratio,
    faces, diagonal_out, residual_out, free_out, term_z,
):
    planes, rows, width = pressure.shape
    lane = lax.broadcasted_iota(jnp.int32, (ROWS, width), 1)
    closed = jnp.zeros((ROWS, width), F32)
    parts = row_parts(rows)

    def plane(z, low, high):
        perms = [perm[z, part] for part in parts]
        values = [pressure[z, part] for part in parts]
        perm_lower, _ = row_shifts(perms, closed, closed)
        lower = [harmonic(*pair) for pair in zip(perms, perm_lower)]
        _, upper = row_shifts(lower, closed, closed)
        value_lower, value_upper = row_shifts(values, closed, closed)
        for at, part in enumerate(parts):
            here, value = perms[at], values[at]
            left = harmonic(here, jnp.where(lane == 0, 0.0, pltpu.roll(here, 1, 1)))
            right = pltpu.roll(left, width - 1, 1)
            terms, views = [None, None], [None, None]
            if low is not None:
                terms[0], views[0] = term_z[z, part], pressure[low, part]
            if high is not None:
                terms[1], views[1] = harmonic(here, perm[high, part]), pressure[high, part]
                term_z[high, part] = terms[1]
            terms += [lower[at], upper[at], left, right]
            views += [value_lower[at], value_upper[at], *lane_shifts(value)]
            storage, biot = storage_of[z, part], biot_of[z, part]
            coupling = biot * ratio[z, part]
            free = 1.0 - fixed[z, part].astype(F32)
            diagonal, neighbours = storage + coupling, None
            for number, (term, view) in enumerate(zip(terms, views)):
                if term is not None:
                    faces[number, z, part] = free * term
                    diagonal = diagonal + term
                    neighbours = term * view if neighbours is None else neighbours + term * view
            right_side = storage * old[z, part] + coupling * value - biot * strain[z, part] + source[z, part]
            diagonal_out[z, part] = diagonal
            residual_out[z, part] = right_side - (diagonal * value - neighbours)
            free_out[z, part] = free

    plane(0, None, 1)
    lax.fori_loop(1, planes - 1, lambda z, c: (plane(z, z - 1, z + 1), c)[1], 0)
    plane(planes - 1, planes - 2, None)


def begin_kernel(
    zones,
    zone, face_table, diagonal_ref, residual_ref, free_ref, pressure, below_z, above_z, y_got, y_got_too,
    inverse, q_out, u_out, face_z, face_y, z_low, z_high, y_first, y_second,
    y_low, y_high,
):
    planes, rows, width = pressure.shape
    inside = inside_flags()
    below_zone, above_zone = as_sides(y_got[0], y_got_too[0])
    below_value, above_value = as_sides(y_got[1], y_got_too[1])
    table = face_table[...]

    def outer_term(own, other, side):
        index = own * zones + other.astype(jnp.int32)
        return look_up(table, jnp.where(inside[side], index, NO_FACE))

    sub = lax.broadcasted_iota(jnp.int32, (ROWS, width), 0)
    ends = (
        (pl.ds(0, 1), below_zone, below_value),
        (pl.ds(rows - 1, 1), above_zone, above_value),
    )
    gain_y = []
    for side, (row, other, value) in enumerate(ends):
        here = jnp.concatenate([zone[z, row] for z in range(planes)], axis=0)
        own = jnp.concatenate([pressure[z, row] for z in range(planes)], axis=0)
        free = jnp.concatenate([free_ref[z, row] for z in range(planes)], axis=0)
        term = outer_term(here, other, 2 + side)
        face_y[side] = free * term
        gain_y.append((term, term * (value - own)))

    def plane(z, outer):
        for part in row_parts(rows):
            diagonal, residual, free = diagonal_ref[z, part], residual_ref[z, part], free_ref[z, part]
            if outer is not None:
                side, halo = outer
                term = outer_term(zone[z, part], halo[0, part], side)
                diagonal = diagonal + term
                residual = residual + term * (halo[1, part] - pressure[z, part])
                face_z[side, part] = free * term
            for side, tile, row in ((0, 0, 0), (1, rows - ROWS, ROWS - 1)):
                if part.start == tile:
                    term, gain = (jnp.broadcast_to(value[z : z + 1], (ROWS, width)) for value in gain_y[side])
                    diagonal = diagonal + jnp.where(sub == row, term, 0.0)
                    residual = residual + jnp.where(sub == row, gain, 0.0)
            reciprocal = 1.0 / diagonal
            residual = free * residual
            precond = residual * reciprocal
            inverse[z, part] = reciprocal
            u_out[z, part] = residual
            q_out[z, part] = precond
            if part.start == 0:
                y_low[z : z + 1] = precond[:1]
            if part.start == rows - ROWS:
                y_high[z : z + 1] = precond[ROWS - 1 :]

    for z in range(planes):
        plane(z, (0, below_z) if z == 0 else (1, above_z) if z == planes - 1 else None)
    z_low[...] = q_out[0]
    z_high[...] = q_out[planes - 1]
    y_first[...], y_second[...] = to_send(y_low[...], y_high[...])


def apply_planes(q_ref, faces, face_z, face_y, below_z, above_z, y_got, y_got_too, emit, carry):
    planes, rows, width = q_ref.shape
    parts = row_parts(rows)
    below_y, above_y = as_sides(y_got[...], y_got_too[...])
    gain = (face_y[0] * below_y, face_y[1] * above_y)
    sub = lax.broadcasted_iota(jnp.int32, (ROWS, width), 0)
    closed = jnp.zeros((ROWS, width), F32)
    for z in range(planes):
        values = [q_ref[z, part] for part in parts]
        lower, upper = row_shifts(values, closed, closed)
        for at, part in enumerate(parts):
            left, right = lane_shifts(values[at])
            if z == 0:
                u = face_z[0, part] * below_z[part] + faces[1, z, part] * q_ref[z + 1, part]
            elif z == planes - 1:
                u = faces[0, z, part] * q_ref[z - 1, part] + face_z[1, part] * above_z[part]
            else:
                u = faces[0, z, part] * q_ref[z - 1, part] + faces[1, z, part] * q_ref[z + 1, part]
            u = u + faces[2, z, part] * lower[at] + faces[3, z, part] * upper[at]
            u = u + faces[4, z, part] * left + faces[5, z, part] * right
            for side, tile, row in ((0, 0, 0), (1, rows - ROWS, ROWS - 1)):
                if part.start == tile:
                    u = u + jnp.where(sub == row, jnp.broadcast_to(gain[side][z : z + 1], (ROWS, width)), 0.0)
            carry = emit(z, part, u, carry)
    return carry


def stage_kernel(
    q_ref, faces, face_z, face_y, inverse, below_z, above_z, y_got, y_got_too,
    q_out, u_out, z_low, z_high, y_first, y_second,
    y_low, y_high,
):
    planes, rows, _ = q_ref.shape

    def emit(z, part, u, carry):
        q = u * inverse[z, part]
        u_out[z, part] = u
        q_out[z, part] = q
        if z == 0:
            z_low[part] = q
        if z == planes - 1:
            z_high[part] = q
        if part.start == 0:
            y_low[z : z + 1] = q[:1]
        if part.start == rows - ROWS:
            y_high[z : z + 1] = q[ROWS - 1 :]
        return carry

    apply_planes(q_ref, faces, face_z, face_y, below_z, above_z, y_got, y_got_too, emit, 0)
    y_first[...], y_second[...] = to_send(y_low[...], y_high[...])


def fold(product):
    total = product[:, :LANES]
    for at in range(LANES, product.shape[1], LANES):
        total = total + product[:, at : at + LANES]
    return total


def gram_kernel(sums, count, *refs):
    us, qs = refs[: count], refs[count : 2 * count]
    ratio, out = refs[2 * count :]
    planes, rows, _ = ratio.shape

    def body(z, totals):
        totals = list(totals)
        for at in range(0, rows, ROWS):
            part = pl.ds(at, ROWS)
            fields = {("u", i): us[i][z, part] for i in range(count)}
            fields |= {("q", i): qs[i][z, part] for i in range(count)}
            weight = ratio[z, part]
            fields |= {("y", i): weight * fields["q", i] for i in range(count)}
            for number, (a, i, b, j) in enumerate(sums):
                totals[number] = totals[number] + fold(fields[a, i] * fields[b, j])
        return tuple(totals)

    zero = jnp.zeros((ROWS, LANES), F32)
    for number, total in enumerate(lax.fori_loop(0, planes, body, (zero,) * len(sums))):
        out[number] = total


def last_kernel(
    q2_ref, faces, face_z, face_y, u0_ref, u1_ref, u2_ref, below_z, above_z, y_got, y_got_too, early, middle, out
):
    us = (u0_ref, u1_ref, u2_ref)

    def emit(z, part, u3, totals):
        fields = {("u", i): us[i][z, part] for i in range(3)}
        fields |= {("u", 3): u3, ("q", 2): q2_ref[z, part]}
        return [
            total + fold(fields[a, i] * fields[b, j]) for total, (a, i, b, j) in zip(totals, LATE)
        ]

    zero = jnp.zeros((ROWS, LANES), F32)
    late = apply_planes(
        q2_ref, faces, face_z, face_y, below_z, above_z, y_got, y_got_too, emit, [zero] * len(LATE)
    )
    lane = lax.broadcasted_iota(jnp.int32, (1, LANES), 1)
    row = jnp.zeros((1, LANES), F32)
    for names, totals in ((EARLY, early), (MIDDLE, middle), (LATE, late)):
        for number, name in enumerate(names):
            row = jnp.where(lane == SUMS.index(name), jnp.sum(totals[number], keepdims=True), row)
    out[...] = jnp.broadcast_to(row, out.shape)


def quadratic(left, table, right):
    total = None
    for i, a in enumerate(left):
        for j, b in enumerate(right):
            if a is None or b is None:
                continue
            term = a * b * table(i, j)
            total = term if total is None else total + term
    return total


def combine(totals, cell_count, iterations=3):
    moment = lambda i, j: totals[i + j]
    drop = lambda i, j: totals[i + j] - totals[i + j + 1]
    zero = jnp.zeros_like(totals[0])
    one = zero + 1.0
    residual, direction, change = [one], [one], []
    inner = moment(0, 0)
    for step in range(iterations):
        curvature = quadratic(direction, drop, direction)
        alive = (inner > 0.0) & (curvature > 0.0)
        size = jnp.where(alive, inner / jnp.where(alive, curvature, 1.0), 0.0)
        change = [c + size * d for c, d in zip(change + [zero], direction)]
        image = [a - b for a, b in zip(direction + [zero], [zero] + direction)]
        residual = [r - size * a for r, a in zip(residual + [zero], image)]
        if step + 1 < iterations:
            following = quadratic(residual, moment, residual)
            noise = quadratic([abs(r) for r in residual], lambda i, j: abs(moment(i, j)), [abs(r) for r in residual])
            following = jnp.where(following > 1e-7 * noise, following, 0.0)
            growth = jnp.where(inner > 0.0, following / jnp.where(inner > 0.0, inner, 1.0), 0.0)
            direction = [z + growth * d for z, d in zip(residual, direction + [zero])]
            inner = following
    at = {name: total for name, total in zip(SUMS, totals)}
    closing = quadratic(residual, lambda i, j: at["u", min(i, j), "u", max(i, j)], residual)
    changed = quadratic(change, lambda i, j: at["y", min(i, j), "y", max(i, j)], change)
    scale = 1.0 / cell_count
    return change, jnp.sqrt(jnp.maximum(closing, 0.0) * scale), jnp.sqrt(jnp.maximum(changed, 0.0) * scale)


def final_kernel(
    cell_count, rows_ref, q0, q1, q2, pressure_ref, strain_ref, ratio, pressure_hbm, strain_hbm, norms_hbm,
    pressure_out, strain_out, norms, sems, norms_sem,
):
    planes, rows, width = pressure_ref.shape
    total = rows_ref[:ROWS]
    for at in range(ROWS, rows_ref.shape[0], ROWS):
        total = total + rows_ref[at : at + ROWS]
    for step in (4, 2, 1):
        total = total + pltpu.roll(total, step, 0)
    totals = [
        jnp.take_along_axis(total, jnp.full((ROWS, LANES), at, jnp.int32), axis=1, mode="promise_in_bounds")
        for at in range(len(SUMS))
    ]
    change, closing, changed = combine(totals, cell_count)
    lane = lax.broadcasted_iota(jnp.int32, (1, LANES), 1)
    norms[...] = jnp.where(lane == 0, closing[:1], changed[:1])[:, :2]
    norms_copy = pltpu.make_async_copy(norms, norms_hbm, norms_sem)
    norms_copy.start()
    weights = [jnp.concatenate([c] * (width // LANES), axis=1) for c in change]

    def copies(z):
        return [
            pltpu.make_async_copy(kept.at[z], whole.at[z], sems.at[number, z])
            for number, (kept, whole) in enumerate(((pressure_out, pressure_hbm), (strain_out, strain_hbm)))
        ]

    for z in range(planes):
        for part in row_parts(rows):
            delta = weights[0] * q0[z, part] + weights[1] * q1[z, part] + weights[2] * q2[z, part]
            pressure_out[z, part] = pressure_ref[z, part] + delta
            strain_out[z, part] = strain_ref[z, part] + ratio[z, part] * delta
        for copy in copies(z):
            copy.start()
    for z in range(planes):
        for copy in copies(z):
            copy.wait()
    norms_copy.wait()


def ring(count, step):
    return [(i, (i + step) % count) for i in range(count)]


def pairs_along_y(count_z, count_y, start):
    pairs = []
    for z in range(count_z):
        partner = list(range(count_y))
        for y in range(start, count_y - 1, 2):
            partner[y], partner[y + 1] = y + 1, y
        pairs += [
            (z * count_y + y, (z if partner[y] != y else z ^ 1) * count_y + partner[y]) for y in range(count_y)
        ]
    return pairs


def exchange(z_low, z_high, y_first, y_second):
    count_z, count_y = lax.axis_size("gz"), lax.axis_size("gy")
    both = ("gz", "gy")
    if paired(count_z, count_y):
        ways = [(both, pairs_along_y(count_z, count_y, start)) for start in (0, 1)]
    else:
        ways = [("gy", ring(count_y, step)) for step in (1, -1)]
    got = {}
    for name, field, axis, pairs in (
        ("send_low", z_low, "gz", ring(count_z, -1)),
        ("send_high", z_high, "gz", ring(count_z, 1)),
        ("send_first", y_first, *ways[0]),
        ("send_second", y_second, *ways[1]),
    ):
        got[name] = lax.ppermute(field, axis, pairs)
    return got["send_high"], got["send_low"], got["send_first"], got["send_second"]


def call(kernel, outs, specs, *operands, scratch=(), out_specs=None):
    results = [pltpu.VMEM(out, F32) if isinstance(out, tuple) else out for out in outs]
    out_specs = out_specs or [VMEM] * len(results)
    operands = [
        pltpu.with_memory_space_constraint(operand, spec.memory_space) for operand, spec in zip(operands, specs)
    ]
    single = len(results) == 1
    return pl.pallas_call(
        kernel,
        out_shape=results[0] if single else results,
        in_specs=specs,
        out_specs=out_specs[0] if single else out_specs,
        scratch_shapes=list(scratch),
        compiler_params=pltpu.CompilerParams(vmem_limit_bytes=16 << 20),
    )(*operands)


def per_device(
    zone_ids, fixed_cells, pressure_old, pressure_iter, strain_change, source,
    zone_perm, zone_storage, zone_biot, zone_bulk,
):
    planes, rows, width = zone_ids.shape
    field = (planes, rows, width)
    sides = ((rows, width), (rows, width), (planes, width), (planes, width))
    devices = lax.axis_size("gz") * lax.axis_size("gy")
    cell_count = zone_ids.size * devices
    line = pltpu.VMEM((planes, width), F32)

    ints = pltpu.VMEM(field, jnp.int32)
    zone, pressure, fixed, old, strain, source, perm, storage, biot, ratio, face_table, *edges = call(
        load_kernel,
        [ints, field, ints, *[field] * 7, (ROWS, LANES), *[(2, *side) for side in sides]], [HBM] * 10,
        zone_ids, pressure_iter, fixed_cells, pressure_old, strain_change, source,
        zone_perm, zone_storage, zone_biot, zone_bulk,
        scratch=[*[pltpu.SMEM(zone_perm.shape, F32)] * 4, pltpu.SemaphoreType.DMA((10,))],
    )
    halo = exchange(*edges)
    faces, diagonal, residual, free = call(
        prepare_kernel, [(6, *field)] + [field] * 3, [VMEM] * 9,
        pressure, fixed, old, strain, source, perm, storage, biot, ratio, scratch=[pltpu.VMEM(field, F32)],
    )
    inverse, q0, u0, face_z, face_y, *edges = call(
        functools.partial(begin_kernel, zone_perm.shape[0]),
        [field, field, field, (2, rows, width), (2, planes, width), *sides], [VMEM] * 10,
        zone, face_table, diagonal, residual, free, pressure, *halo, scratch=[line, line],
    )
    parts = (faces, face_z, face_y)
    halo = exchange(*edges)
    q1, u1, *edges = call(
        stage_kernel, [field, field, *sides], [VMEM] * 9, q0, *parts, inverse, *halo, scratch=[line, line]
    )
    halo = exchange(*edges)
    early = call(
        functools.partial(gram_kernel, EARLY, 2), [(len(EARLY), ROWS, LANES)], [VMEM] * 5,
        u0, u1, q0, q1, ratio,
    )
    q2, u2, *edges = call(
        stage_kernel, [field, field, *sides], [VMEM] * 9, q1, *parts, inverse, *halo, scratch=[line, line]
    )
    halo = exchange(*edges)
    middle = call(
        functools.partial(gram_kernel, MIDDLE, 3), [(len(MIDDLE), ROWS, LANES)], [VMEM] * 7,
        u0, u1, u2, q0, q1, q2, ratio,
    )
    sums = call(
        last_kernel, [(devices, LANES)], [VMEM] * 13,
        q2, *parts, u0, u1, u2, *halo, early, middle,
    )
    gathered = lax.all_to_all(sums, ("gz", "gy"), 0, 0, tiled=True)
    pressure_next, strain_next, norms = call(
        functools.partial(final_kernel, cell_count),
        [jax.ShapeDtypeStruct(shape, F32) for shape in (field, field, (1, 2))], [VMEM] * 7,
        gathered, q0, q1, q2, pressure, strain, ratio, out_specs=[HBM] * 3,
        scratch=[
            *[pltpu.VMEM(field, F32)] * 2, pltpu.VMEM((1, 2), F32), pltpu.SemaphoreType.DMA((2, planes)),
            pltpu.SemaphoreType.DMA,
        ],
    )
    return pressure_next, strain_next, norms.reshape(2)


def solution(mesh):
    split = P("gz", "gy", None)
    return jax.shard_map(
        per_device,
        mesh=mesh,
        in_specs=(split,) * 6 + (P(),) * 4,
        out_specs=(split, split, P()),
        check_vma=False,
    )
```

```python
import functools

import jax
import jax.numpy as jnp
from jax import lax
from jax.experimental import pallas as pl
from jax.experimental.pallas import tpu as pltpu
from jax.sharding import PartitionSpec as P

F32 = jnp.float32
ROWS = 8
LANES = 128
VMEM = pl.BlockSpec(memory_space=pltpu.VMEM)
HBM = pl.BlockSpec(memory_space=pltpu.HBM)

MOMENTS = (("q", 0, "u", 0), ("q", 0, "u", 1), ("q", 1, "u", 1), ("q", 1, "u", 2), ("q", 2, "u", 2), ("q", 2, "u", 3))
CLOSING = tuple(("u", i, "u", j) for i in range(4) for j in range(i, 4))
CHANGE = tuple(("y", i, "y", j) for i in range(3) for j in range(i, 3))
SUMS = MOMENTS + CLOSING + CHANGE
EARLY = tuple(s for s in SUMS if max(s[1], s[3]) <= 1)
MIDDLE = tuple(s for s in SUMS if max(s[1], s[3]) == 2)
LATE = tuple(s for s in SUMS if max(s[1], s[3]) == 3)


def table_row(table_ref):
    lane = lax.broadcasted_iota(jnp.int32, (ROWS, LANES), 1)
    row = jnp.zeros((ROWS, LANES), F32)
    for zone in range(table_ref.shape[0]):
        row = jnp.where(lane == zone, table_ref[zone], row)
    return row


def look_up(row, zones):
    parts = [
        jnp.take_along_axis(row, zones[:, at : at + LANES], axis=1, mode="promise_in_bounds")
        for at in range(0, zones.shape[1], LANES)
    ]
    return jnp.concatenate(parts, axis=1)


def zone_bits(zones, count):
    return [(zones & (1 << bit)) != 0 for bit in range(max(count - 1, 1).bit_length())]


def pick(bits, entries):
    entries = list(entries) + [entries[-1]] * (2 ** len(bits) - len(entries))
    for bit in bits:
        entries = [jnp.where(bit, odd, even) for even, odd in zip(entries[::2], entries[1::2])]
    return entries[0]


def harmonic(lower_side, upper_side):
    return 2.0 * lower_side * upper_side / (lower_side + upper_side)


def row_shifts(tiles, before, after):
    sub = lax.broadcasted_iota(jnp.int32, tiles[0].shape, 0)
    down = [pltpu.roll(tile, 1, 0) for tile in tiles]
    up = [pltpu.roll(tile, ROWS - 1, 0) for tile in tiles]
    lower, upper = [], []
    for at in range(len(tiles)):
        lower.append(jnp.where(sub == 0, down[at - 1] if at else before, down[at]))
        upper.append(jnp.where(sub == ROWS - 1, up[at + 1] if at + 1 < len(tiles) else after, up[at]))
    return lower, upper


def lane_shifts(tile):
    width = tile.shape[1]
    return pltpu.roll(tile, 1, 1), pltpu.roll(tile, width - 1, 1)


def paired(count_z, count_y):
    return count_z % 2 == 0 and count_y % 2 == 0


def to_send(low, high):
    if not paired(lax.axis_size("gz"), lax.axis_size("gy")):
        return high, low
    odd = lax.rem(lax.axis_index("gy"), 2) == 1
    return jnp.where(odd, low, high), jnp.where(odd, high, low)


def as_sides(first, second):
    if not paired(lax.axis_size("gz"), lax.axis_size("gy")):
        return first, second
    odd = lax.rem(lax.axis_index("gy"), 2) == 1
    return jnp.where(odd, first, second), jnp.where(odd, second, first)


def inside_flags():
    flags = []
    for axis in ("gz", "gy"):
        place = lax.axis_index(axis)
        flags += [place > 0, place < lax.axis_size(axis) - 1]
    return flags


def row_parts(rows):
    return [pl.ds(at, ROWS) for at in range(0, rows, ROWS)]


NO_FACE = LANES - 1


def face_row(perm_row, zones):
    lane = lax.broadcasted_iota(jnp.int32, (ROWS, LANES), 1)
    known = lane < zones * zones
    pair = jnp.where(known, lane, 0)
    sides = [
        jnp.take_along_axis(perm_row, side, axis=1, mode="promise_in_bounds")
        for side in (lax.div(pair, zones), lax.rem(pair, zones))
    ]
    return jnp.where(known, harmonic(*sides), 0.0)


def load_kernel(
    zone_hbm, pressure_hbm, perm_hbm, storage_hbm, biot_hbm, bulk_hbm,
    zone, pressure, values_of, face_table, z_low, z_high, y_first, y_second,
    perm_table, storage_table, biot_table, bulk_table, sems,
):
    planes, rows, _ = zone.shape
    copies = [
        pltpu.make_async_copy(*pair, sems.at[number])
        for number, pair in enumerate((
            (perm_hbm, perm_table), (storage_hbm, storage_table), (biot_hbm, biot_table), (bulk_hbm, bulk_table),
            (zone_hbm, zone), (pressure_hbm, pressure),
        ))
    ]
    for copy in copies:
        copy.start()
    for copy in copies[:4]:
        copy.wait()
    zones = perm_table.shape[0]
    face_table[...] = face_row(table_row(perm_table), zones)
    one = jnp.ones((ROWS, LANES), F32)
    for number in range(zones):
        for at, table in enumerate((perm_table, storage_table, biot_table)):
            values_of[at * zones + number] = table[number] * one
        values_of[3 * zones + number] = biot_table[number] * one / (bulk_table[number] * one)
    for copy in copies[4:]:
        copy.wait()
    faces_y = []
    for side, out in enumerate((z_low, z_high)):
        plane = (0, planes - 1)[side]
        out[0] = zone[plane].astype(F32)
        out[1] = pressure[plane]
        row = pl.ds((0, rows - 1)[side], 1)
        ids = jnp.concatenate([zone[z, row] for z in range(planes)], axis=0)
        values = jnp.concatenate([pressure[z, row] for z in range(planes)], axis=0)
        faces_y.append((ids.astype(F32), values))
    for number in range(2):
        y_first[number], y_second[number] = to_send(faces_y[0][number], faces_y[1][number])


def prepare_kernel(
    zone, pressure, values_of, fixed_hbm, old_hbm, strain_hbm, source_hbm,
    faces, diagonal_out, residual_out, free_out, ratio, strain,
    fixed, old, source, perm, storage_of, biot_of, term_z, sems,
):
    planes, rows, width = pressure.shape
    pairs = ((fixed_hbm, fixed), (old_hbm, old), (strain_hbm, strain), (source_hbm, source))
    copies = [pltpu.make_async_copy(*pair, sems.at[number]) for number, pair in enumerate(pairs)]
    for copy in copies:
        copy.start()
    zones = values_of.shape[0] // 4
    entries = [
        [jnp.concatenate([values_of[at * zones + number]] * (width // LANES), axis=1) for number in range(zones)]
        for at in range(4)
    ]

    def fill(z, carry):
        for part in row_parts(rows):
            bits = zone_bits(zone[z, part], zones)
            for out, entry in zip((perm, storage_of, biot_of, ratio), entries):
                out[z, part] = pick(bits, entry)
        return carry

    lax.fori_loop(0, planes, fill, 0)
    for copy in copies:
        copy.wait()
    lane = lax.broadcasted_iota(jnp.int32, (ROWS, width), 1)
    closed = jnp.zeros((ROWS, width), F32)
    parts = row_parts(rows)

    def plane(z, low, high):
        perms = [perm[z, part] for part in parts]
        values = [pressure[z, part] for part in parts]
        perm_lower, _ = row_shifts(perms, closed, closed)
        lower = [harmonic(*pair) for pair in zip(perms, perm_lower)]
        _, upper = row_shifts(lower, closed, closed)
        value_lower, value_upper = row_shifts(values, closed, closed)
        for at, part in enumerate(parts):
            here, value = perms[at], values[at]
            left = harmonic(here, jnp.where(lane == 0, 0.0, pltpu.roll(here, 1, 1)))
            right = pltpu.roll(left, width - 1, 1)
            terms, views = [None, None], [None, None]
            if low is not None:
                terms[0], views[0] = term_z[z, part], pressure[low, part]
            if high is not None:
                terms[1], views[1] = harmonic(here, perm[high, part]), pressure[high, part]
                term_z[high, part] = terms[1]
            terms += [lower[at], upper[at], left, right]
            views += [value_lower[at], value_upper[at], *lane_shifts(value)]
            storage, biot = storage_of[z, part], biot_of[z, part]
            coupling = biot * ratio[z, part]
            free = 1.0 - fixed[z, part].astype(F32)
            diagonal, neighbours = storage + coupling, None
            for number, (term, view) in enumerate(zip(terms, views)):
                if term is not None:
                    faces[number, z, part] = free * term
                    diagonal = diagonal + term
                    neighbours = term * view if neighbours is None else neighbours + term * view
            right_side = storage * old[z, part] + coupling * value - biot * strain[z, part] + source[z, part]
            diagonal_out[z, part] = diagonal
            residual_out[z, part] = right_side - (diagonal * value - neighbours)
            free_out[z, part] = free

    plane(0, None, 1)
    lax.fori_loop(1, planes - 1, lambda z, c: (plane(z, z - 1, z + 1), c)[1], 0)
    plane(planes - 1, planes - 2, None)


def begin_kernel(
    zones,
    zone, face_table, diagonal_ref, residual_ref, free_ref, pressure, below_z, above_z, y_got, y_got_too,
    inverse, q_out, u_out, face_z, face_y, z_low, z_high, y_first, y_second,
    y_low, y_high,
):
    planes, rows, width = pressure.shape
    inside = inside_flags()
    below_zone, above_zone = as_sides(y_got[0], y_got_too[0])
    below_value, above_value = as_sides(y_got[1], y_got_too[1])
    table = face_table[...]

    def outer_term(own, other, side):
        index = own * zones + other.astype(jnp.int32)
        return look_up(table, jnp.where(inside[side], index, NO_FACE))

    sub = lax.broadcasted_iota(jnp.int32, (ROWS, width), 0)
    ends = (
        (pl.ds(0, 1), below_zone, below_value),
        (pl.ds(rows - 1, 1), above_zone, above_value),
    )
    gain_y = []
    for side, (row, other, value) in enumerate(ends):
        here = jnp.concatenate([zone[z, row] for z in range(planes)], axis=0)
        own = jnp.concatenate([pressure[z, row] for z in range(planes)], axis=0)
        free = jnp.concatenate([free_ref[z, row] for z in range(planes)], axis=0)
        term = outer_term(here, other, 2 + side)
        face_y[side] = free * term
        gain_y.append((term, term * (value - own)))

    def plane(z, outer):
        for part in row_parts(rows):
            diagonal, residual, free = diagonal_ref[z, part], residual_ref[z, part], free_ref[z, part]
            if outer is not None:
                side, halo = outer
                term = outer_term(zone[z, part], halo[0, part], side)
                diagonal = diagonal + term
                residual = residual + term * (halo[1, part] - pressure[z, part])
                face_z[side, part] = free * term
            for side, tile, row in ((0, 0, 0), (1, rows - ROWS, ROWS - 1)):
                if part.start == tile:
                    term, gain = (jnp.broadcast_to(value[z : z + 1], (ROWS, width)) for value in gain_y[side])
                    diagonal = diagonal + jnp.where(sub == row, term, 0.0)
                    residual = residual + jnp.where(sub == row, gain, 0.0)
            reciprocal = 1.0 / diagonal
            residual = free * residual
            precond = residual * reciprocal
            inverse[z, part] = reciprocal
            u_out[z, part] = residual
            q_out[z, part] = precond
            if part.start == 0:
                y_low[z : z + 1] = precond[:1]
            if part.start == rows - ROWS:
                y_high[z : z + 1] = precond[ROWS - 1 :]

    for z in range(planes):
        plane(z, (0, below_z) if z == 0 else (1, above_z) if z == planes - 1 else None)
    z_low[...] = q_out[0]
    z_high[...] = q_out[planes - 1]
    y_first[...], y_second[...] = to_send(y_low[...], y_high[...])


def apply_planes(q_ref, faces, face_z, face_y, below_z, above_z, y_got, y_got_too, emit, carry):
    planes, rows, width = q_ref.shape
    parts = row_parts(rows)
    below_y, above_y = as_sides(y_got[...], y_got_too[...])
    gain = (face_y[0] * below_y, face_y[1] * above_y)
    sub = lax.broadcasted_iota(jnp.int32, (ROWS, width), 0)
    closed = jnp.zeros((ROWS, width), F32)
    for z in range(planes):
        values = [q_ref[z, part] for part in parts]
        lower, upper = row_shifts(values, closed, closed)
        for at, part in enumerate(parts):
            left, right = lane_shifts(values[at])
            if z == 0:
                u = face_z[0, part] * below_z[part] + faces[1, z, part] * q_ref[z + 1, part]
            elif z == planes - 1:
                u = faces[0, z, part] * q_ref[z - 1, part] + face_z[1, part] * above_z[part]
            else:
                u = faces[0, z, part] * q_ref[z - 1, part] + faces[1, z, part] * q_ref[z + 1, part]
            u = u + faces[2, z, part] * lower[at] + faces[3, z, part] * upper[at]
            u = u + faces[4, z, part] * left + faces[5, z, part] * right
            for side, tile, row in ((0, 0, 0), (1, rows - ROWS, ROWS - 1)):
                if part.start == tile:
                    u = u + jnp.where(sub == row, jnp.broadcast_to(gain[side][z : z + 1], (ROWS, width)), 0.0)
            carry = emit(z, part, u, carry)
    return carry


def stage_kernel(
    q_ref, faces, face_z, face_y, inverse, below_z, above_z, y_got, y_got_too,
    q_out, u_out, z_low, z_high, y_first, y_second,
    y_low, y_high,
):
    planes, rows, _ = q_ref.shape

    def emit(z, part, u, carry):
        q = u * inverse[z, part]
        u_out[z, part] = u
        q_out[z, part] = q
        if z == 0:
            z_low[part] = q
        if z == planes - 1:
            z_high[part] = q
        if part.start == 0:
            y_low[z : z + 1] = q[:1]
        if part.start == rows - ROWS:
            y_high[z : z + 1] = q[ROWS - 1 :]
        return carry

    apply_planes(q_ref, faces, face_z, face_y, below_z, above_z, y_got, y_got_too, emit, 0)
    y_first[...], y_second[...] = to_send(y_low[...], y_high[...])


def fold(product):
    total = product[:, :LANES]
    for at in range(LANES, product.shape[1], LANES):
        total = total + product[:, at : at + LANES]
    return total


def gram_kernel(sums, count, *refs):
    us, qs = refs[: count], refs[count : 2 * count]
    ratio, out = refs[2 * count :]
    planes, rows, _ = ratio.shape

    def body(z, totals):
        totals = list(totals)
        for at in range(0, rows, ROWS):
            part = pl.ds(at, ROWS)
            fields = {("u", i): us[i][z, part] for i in range(count)}
            fields |= {("q", i): qs[i][z, part] for i in range(count)}
            weight = ratio[z, part]
            fields |= {("y", i): weight * fields["q", i] for i in range(count)}
            for number, (a, i, b, j) in enumerate(sums):
                totals[number] = totals[number] + fold(fields[a, i] * fields[b, j])
        return tuple(totals)

    zero = jnp.zeros((ROWS, LANES), F32)
    for number, total in enumerate(lax.fori_loop(0, planes, body, (zero,) * len(sums))):
        out[number] = total


def last_kernel(
    q2_ref, faces, face_z, face_y, u0_ref, u1_ref, u2_ref, below_z, above_z, y_got, y_got_too, early, middle, out
):
    us = (u0_ref, u1_ref, u2_ref)

    def emit(z, part, u3, totals):
        fields = {("u", i): us[i][z, part] for i in range(3)}
        fields |= {("u", 3): u3, ("q", 2): q2_ref[z, part]}
        return [
            total + fold(fields[a, i] * fields[b, j]) for total, (a, i, b, j) in zip(totals, LATE)
        ]

    zero = jnp.zeros((ROWS, LANES), F32)
    late = apply_planes(
        q2_ref, faces, face_z, face_y, below_z, above_z, y_got, y_got_too, emit, [zero] * len(LATE)
    )
    lane = lax.broadcasted_iota(jnp.int32, (1, LANES), 1)
    row = jnp.zeros((1, LANES), F32)
    for names, totals in ((EARLY, early), (MIDDLE, middle), (LATE, late)):
        for number, name in enumerate(names):
            row = jnp.where(lane == SUMS.index(name), jnp.sum(totals[number], keepdims=True), row)
    out[...] = jnp.broadcast_to(row, out.shape)


def quadratic(left, table, right):
    total = None
    for i, a in enumerate(left):
        for j, b in enumerate(right):
            if a is None or b is None:
                continue
            term = a * b * table(i, j)
            total = term if total is None else total + term
    return total


def combine(totals, cell_count, iterations=3):
    moment = lambda i, j: totals[i + j]
    drop = lambda i, j: totals[i + j] - totals[i + j + 1]
    zero = jnp.zeros_like(totals[0])
    one = zero + 1.0
    residual, direction, change = [one], [one], []
    inner = moment(0, 0)
    for step in range(iterations):
        curvature = quadratic(direction, drop, direction)
        alive = (inner > 0.0) & (curvature > 0.0)
        size = jnp.where(alive, inner / jnp.where(alive, curvature, 1.0), 0.0)
        change = [c + size * d for c, d in zip(change + [zero], direction)]
        image = [a - b for a, b in zip(direction + [zero], [zero] + direction)]
        residual = [r - size * a for r, a in zip(residual + [zero], image)]
        if step + 1 < iterations:
            following = quadratic(residual, moment, residual)
            noise = quadratic([abs(r) for r in residual], lambda i, j: abs(moment(i, j)), [abs(r) for r in residual])
            following = jnp.where(following > 1e-7 * noise, following, 0.0)
            growth = jnp.where(inner > 0.0, following / jnp.where(inner > 0.0, inner, 1.0), 0.0)
            direction = [z + growth * d for z, d in zip(residual, direction + [zero])]
            inner = following
    at = {name: total for name, total in zip(SUMS, totals)}
    closing = quadratic(residual, lambda i, j: at["u", min(i, j), "u", max(i, j)], residual)
    changed = quadratic(change, lambda i, j: at["y", min(i, j), "y", max(i, j)], change)
    scale = 1.0 / cell_count
    return change, jnp.sqrt(jnp.maximum(closing, 0.0) * scale), jnp.sqrt(jnp.maximum(changed, 0.0) * scale)


def final_kernel(
    cell_count, rows_ref, q0, q1, q2, pressure_ref, strain_ref, ratio, pressure_hbm, strain_hbm, norms_hbm,
    pressure_out, strain_out, norms, sems, norms_sem,
):
    planes, rows, width = pressure_ref.shape
    total = rows_ref[:ROWS]
    for at in range(ROWS, rows_ref.shape[0], ROWS):
        total = total + rows_ref[at : at + ROWS]
    for step in (4, 2, 1):
        total = total + pltpu.roll(total, step, 0)
    totals = [
        jnp.take_along_axis(total, jnp.full((ROWS, LANES), at, jnp.int32), axis=1, mode="promise_in_bounds")
        for at in range(len(SUMS))
    ]
    change, closing, changed = combine(totals, cell_count)
    lane = lax.broadcasted_iota(jnp.int32, (1, LANES), 1)
    norms[...] = jnp.where(lane == 0, closing[:1], changed[:1])[:, :2]
    norms_copy = pltpu.make_async_copy(norms, norms_hbm, norms_sem)
    norms_copy.start()
    weights = [jnp.concatenate([c] * (width // LANES), axis=1) for c in change]

    def copies(z):
        return [
            pltpu.make_async_copy(kept.at[z], whole.at[z], sems.at[number, z])
            for number, (kept, whole) in enumerate(((pressure_out, pressure_hbm), (strain_out, strain_hbm)))
        ]

    for z in range(planes):
        for part in row_parts(rows):
            delta = weights[0] * q0[z, part] + weights[1] * q1[z, part] + weights[2] * q2[z, part]
            pressure_out[z, part] = pressure_ref[z, part] + delta
            strain_out[z, part] = strain_ref[z, part] + ratio[z, part] * delta
        for copy in copies(z):
            copy.start()
    for z in range(planes):
        for copy in copies(z):
            copy.wait()
    norms_copy.wait()


def ring(count, step):
    return [(i, (i + step) % count) for i in range(count)]


def pairs_along_y(count_z, count_y, start):
    pairs = []
    for z in range(count_z):
        partner = list(range(count_y))
        for y in range(start, count_y - 1, 2):
            partner[y], partner[y + 1] = y + 1, y
        pairs += [
            (z * count_y + y, (z if partner[y] != y else z ^ 1) * count_y + partner[y]) for y in range(count_y)
        ]
    return pairs


def exchange(z_low, z_high, y_first, y_second):
    count_z, count_y = lax.axis_size("gz"), lax.axis_size("gy")
    both = ("gz", "gy")
    if paired(count_z, count_y):
        ways = [(both, pairs_along_y(count_z, count_y, start)) for start in (0, 1)]
    else:
        ways = [("gy", ring(count_y, step)) for step in (1, -1)]
    got = {}
    for name, field, axis, pairs in (
        ("send_low", z_low, "gz", ring(count_z, -1)),
        ("send_high", z_high, "gz", ring(count_z, 1)),
        ("send_first", y_first, *ways[0]),
        ("send_second", y_second, *ways[1]),
    ):
        got[name] = lax.ppermute(field, axis, pairs)
    return got["send_high"], got["send_low"], got["send_first"], got["send_second"]


def call(kernel, outs, specs, *operands, scratch=(), out_specs=None):
    results = [pltpu.VMEM(out, F32) if isinstance(out, tuple) else out for out in outs]
    out_specs = out_specs or [VMEM] * len(results)
    operands = [
        pltpu.with_memory_space_constraint(operand, spec.memory_space) for operand, spec in zip(operands, specs)
    ]
    single = len(results) == 1
    return pl.pallas_call(
        kernel,
        out_shape=results[0] if single else results,
        in_specs=specs,
        out_specs=out_specs[0] if single else out_specs,
        scratch_shapes=list(scratch),
        compiler_params=pltpu.CompilerParams(vmem_limit_bytes=16 << 20),
    )(*operands)


def per_device(
    zone_ids, fixed_cells, pressure_old, pressure_iter, strain_change, source,
    zone_perm, zone_storage, zone_biot, zone_bulk,
):
    planes, rows, width = zone_ids.shape
    field = (planes, rows, width)
    sides = ((rows, width), (rows, width), (planes, width), (planes, width))
    devices = lax.axis_size("gz") * lax.axis_size("gy")
    cell_count = zone_ids.size * devices
    line = pltpu.VMEM((planes, width), F32)

    ints = pltpu.VMEM(field, jnp.int32)
    zones = zone_perm.shape[0]
    zone, pressure, values_of, face_table, *edges = call(
        load_kernel,
        [ints, field, (4 * zones, ROWS, LANES), (ROWS, LANES), *[(2, *side) for side in sides]], [HBM] * 6,
        zone_ids, pressure_iter, zone_perm, zone_storage, zone_biot, zone_bulk,
        scratch=[*[pltpu.SMEM((zones,), F32)] * 4, pltpu.SemaphoreType.DMA((6,))],
    )
    halo = exchange(*edges)
    faces, diagonal, residual, free, ratio, strain = call(
        prepare_kernel, [(6, *field)] + [field] * 5, [VMEM] * 3 + [HBM] * 4,
        zone, pressure, values_of, fixed_cells, pressure_old, strain_change, source,
        scratch=[ints, *[pltpu.VMEM(field, F32)] * 6, pltpu.SemaphoreType.DMA((4,))],
    )
    inverse, q0, u0, face_z, face_y, *edges = call(
        functools.partial(begin_kernel, zone_perm.shape[0]),
        [field, field, field, (2, rows, width), (2, planes, width), *sides], [VMEM] * 10,
        zone, face_table, diagonal, residual, free, pressure, *halo, scratch=[line, line],
    )
    parts = (faces, face_z, face_y)
    halo = exchange(*edges)
    q1, u1, *edges = call(
        stage_kernel, [field, field, *sides], [VMEM] * 9, q0, *parts, inverse, *halo, scratch=[line, line]
    )
    halo = exchange(*edges)
    early = call(
        functools.partial(gram_kernel, EARLY, 2), [(len(EARLY), ROWS, LANES)], [VMEM] * 5,
        u0, u1, q0, q1, ratio,
    )
    q2, u2, *edges = call(
        stage_kernel, [field, field, *sides], [VMEM] * 9, q1, *parts, inverse, *halo, scratch=[line, line]
    )
    halo = exchange(*edges)
    middle = call(
        functools.partial(gram_kernel, MIDDLE, 3), [(len(MIDDLE), ROWS, LANES)], [VMEM] * 7,
        u0, u1, u2, q0, q1, q2, ratio,
    )
    sums = call(
        last_kernel, [(devices, LANES)], [VMEM] * 13,
        q2, *parts, u0, u1, u2, *halo, early, middle,
    )
    gathered = lax.all_to_all(sums, ("gz", "gy"), 0, 0, tiled=True)
    pressure_next, strain_next, norms = call(
        functools.partial(final_kernel, cell_count),
        [jax.ShapeDtypeStruct(shape, F32) for shape in (field, field, (1, 2))], [VMEM] * 7,
        gathered, q0, q1, q2, pressure, strain, ratio, out_specs=[HBM] * 3,
        scratch=[
            *[pltpu.VMEM(field, F32)] * 2, pltpu.VMEM((1, 2), F32), pltpu.SemaphoreType.DMA((2, planes)),
            pltpu.SemaphoreType.DMA,
        ],
    )
    return pressure_next, strain_next, norms.reshape(2)


def solution(mesh):
    split = P("gz", "gy", None)
    return jax.shard_map(
        per_device,
        mesh=mesh,
        in_specs=(split,) * 6 + (P(),) * 4,
        out_specs=(split, split, P()),
        check_vma=False,
    )
```
